128 devices in a mesh: atm: 8 (over z, core), land: 16 (over x, y).
Axes of the slice: x: 4, y: 4, z: 4, core: 2. Of those that a mesh axis runs over, the one named last changes fastest.
Arguments:
- tile_forcing: bfloat16 [16384, 128], P(('atm', 'land')), may hold values from -6 to 6
- elevation_gap: float32 [262144], P(('atm', 'land')), may hold values from -5 to 5
- lapse_rate: float32 [128], replicated, may hold values from -3 to 3
- column_tile: int32 [262144], P(('atm', 'land')), may hold values from 0 to 127
- column_target: int32 [262144], P(('atm', 'land')), may hold values from 0 to 655359, as said below
- owner_counts: int32 [128], P(('atm', 'land')), may hold values from 1 to 5120, as said below
- land_state: float32 [655360, 128], P(('atm', 'land')), may hold values from -6 to 6
- w_in: bfloat16 [256, 1024], replicated, may hold values from -0.375 to 0.375
- norm_gains: float32 [2, 1024], replicated, may hold values from 0.5 to 1.5
- w_up: bfloat16 [1, 1024, 1024], replicated, may hold values from -0.1875 to 0.1875
- w_down: bfloat16 [1, 1024, 1024], replicated, may hold values from -0.1875 to 0.1875
- w_out: bfloat16 [1024, 256], replicated, may hold values from -0.1875 to 0.1875
Outputs:
- new_state: float32 [655360, 128], P(('atm', 'land'))
- tile_flux: float32 [16384, 128], P(('atm', 'land'))
The draws below stay inside these ranges and needn't reach their ends.
Inputs may be any that keep to these rules, and one draw needn't show every extreme that they name: `column_target`: live slots of owner j are j * 5120 to j * 5120 + owner_counts[j] - 1; every live slot is named by exactly one column and no other slot is named. The columns of one device name at most 41 slots of any one owner, and some pair reaches 41. `owner_counts`: they sum to 262144; the largest is exactly 5120. `column_tile`: index of the column's tile among the 128 tiles of the device that holds the column.
All inputs are finite; a program needn't handle non-finite values.
Results may differ from the reference program's by a relative error of at most 0.0038.
Values may be sent and summed in bfloat16 or wider, within the bound.
A program may use at most 128 MiB of HBM per device.

```python
import jax
import jax.numpy as jnp
from jax import lax

FORCING = 128
STATE = 128
FLUX = 128
HIDDEN_SIZE = 1024
LAYERS = 1
A_COLS = 2048
TILE_DEV = 128
FEATURES = 256
CAP = 5120
COLS = 262144
SLOTS = 655360
TILES = 16384


def routing_tables(key):
    base = jax.random.fold_in(key, 7321)
    owners = COLS // A_COLS
    middle = A_COLS // owners
    most = 5 * middle // 2
    busy = owners // 8
    order = jax.random.permutation(jax.random.fold_in(base, 1), owners)
    placing = jnp.zeros((owners,), jnp.int32).at[order].set(jnp.arange(owners, dtype=jnp.int32))
    is_busy = placing < busy
    others = owners - busy
    extra = busy * (most - middle)
    lowered = extra // others + (placing - busy < extra % others).astype(jnp.int32)
    share = jnp.where(is_busy, most, middle - lowered).astype(jnp.int32)
    bump = jnp.where(is_busy, 1, jnp.where((placing >= busy) & (placing < 2 * busy), -1, 0)).astype(jnp.int32)
    sender_order = jax.random.permutation(jax.random.fold_in(base, 2), owners)
    signs = jnp.where(sender_order < owners // 2, 1, -1).astype(jnp.int32)
    load = share[None, :] + signs[:, None] * bump[None, :]
    offsets = jnp.cumsum(load, axis=0) - load
    ends = jnp.cumsum(load, axis=1)
    starts = ends - load

    def one_sender(sender):
        position = jnp.arange(A_COLS, dtype=jnp.int32)
        receiver = jnp.sum((ends[sender][None, :] <= position[:, None]).astype(jnp.int32), axis=1)
        within = position - starts[sender][receiver]
        target = receiver * CAP + offsets[sender][receiver] + within
        shuffle = jax.random.permutation(jax.random.fold_in(jax.random.fold_in(base, 3), sender), A_COLS)
        return target[shuffle].astype(jnp.int32)
    targets = lax.map(one_sender, jnp.arange(owners, dtype=jnp.int32))
    return (targets.reshape(COLS), (owners * share).astype(jnp.int32))


def draw_column_target(key, part):
    return routing_tables(key)[0]


def draw_owner_counts(key, part):
    return routing_tables(key)[1]


def touch_ends(entries, rng, smallest, top_value):
    place = [jax.random.randint(jax.random.fold_in(rng, axis), (), 0, length) for axis, length in enumerate(entries.shape)]
    longest = entries.shape.index(max(entries.shape))
    neighbour = place[:longest] + [(place[longest] + 1) % entries.shape[longest]] + place[longest + 1:]
    return entries.at[tuple(place)].set(smallest).at[tuple(neighbour)].set(top_value)


def steps_of(stream_key, dims, split, least, largest):
    loudness, own = 1.0, jax.random.fold_in(stream_key, 6)
    for dim, shards_of in split:
        draws = jnp.exp(jax.random.uniform(jax.random.fold_in(own, dim), (shards_of,), jnp.float32, least / len(split), largest / len(split)))
        loudness = loudness * jnp.repeat(draws, dims[dim] // shards_of).reshape([-1 if axis == dim else 1 for axis in range(len(dims))])
    return loudness


def noise(own_key, extent, spread, reach, pieces=(), kind=jnp.bfloat16):
    loudness = steps_of(own_key, extent, pieces, -0.22, 0.18) if pieces else 1.0
    entries = jax.random.normal(own_key, extent, jnp.float32) * spread * loudness
    return jnp.minimum(jnp.maximum(entries, -reach), reach).astype(kind)


def setup_inputs(seed: int = 0) -> dict:
    seeds = jax.random.split(jax.random.key(seed), 13)
    return {
        "tile_forcing": noise(seeds[0], (TILES, FORCING), 1.0, 6.0, ((0, 128),)),
        "elevation_gap": noise(seeds[1], (COLS,), 1.0, 5.0, ((0, 128),), jnp.float32),
        "lapse_rate": noise(seeds[2], (FORCING,), 0.6, 3.0, (), jnp.float32),
        "column_tile": touch_ends(jax.random.randint(seeds[3], (COLS,), 0, TILE_DEV), jax.random.fold_in(seeds[3], 1), 0, TILE_DEV - 1).astype(jnp.int32),
        "column_target": draw_column_target(jax.random.fold_in(seeds[12], 71), 0),
        "owner_counts": draw_owner_counts(jax.random.fold_in(seeds[12], 71), 0),
        "land_state": noise(seeds[6], (SLOTS, STATE), 1.0, 6.0, ((0, 128),), jnp.float32),
        "w_in": noise(seeds[7], (FEATURES, HIDDEN_SIZE), FEATURES ** -0.5, 0.375),
        "norm_gains": jnp.clip(1.0 + 0.1 * jax.random.normal(seeds[8], (LAYERS + 1, HIDDEN_SIZE), jnp.float32), 0.5, 1.5),
        "w_up": noise(seeds[9], (LAYERS, HIDDEN_SIZE, HIDDEN_SIZE), HIDDEN_SIZE ** -0.5, 0.1875),
        "w_down": noise(seeds[10], (LAYERS, HIDDEN_SIZE, HIDDEN_SIZE), HIDDEN_SIZE ** -0.5, 0.1875),
        "w_out": noise(seeds[11], (HIDDEN_SIZE, STATE + FLUX), HIDDEN_SIZE ** -0.5, 0.1875),
    }


def normed(hidden, gain):
    scale = lax.rsqrt(lax.optimization_barrier(jnp.mean(hidden * hidden, axis=-1, keepdims=True)) + 1e-06)
    return hidden * scale * gain

def network(inputs, w_in, norm_gains, w_up, w_down, w_out):
    hidden = jnp.dot(inputs, w_in, preferred_element_type=jnp.float32)
    for layer in range(w_up.shape[0]):
        lowered = normed(hidden, norm_gains[layer]).astype(jnp.bfloat16)
        active = jax.nn.silu(jnp.dot(lowered, w_up[layer], preferred_element_type=jnp.float32)).astype(jnp.bfloat16)
        hidden = hidden + jnp.dot(active, w_down[layer], preferred_element_type=jnp.float32)
    lowered = normed(hidden, norm_gains[w_up.shape[0]]).astype(jnp.bfloat16)
    return jnp.dot(lowered, w_out, preferred_element_type=jnp.float32).astype(jnp.bfloat16)

def reference(tile_forcing, elevation_gap, lapse_rate, column_tile, column_target, owner_counts, land_state, w_in, norm_gains, w_up, w_down, w_out):
    column_index = jnp.arange(COLS, dtype=jnp.int32)
    tile_of = (column_tile + column_index // A_COLS * TILE_DEV).astype(jnp.int32)
    column_forcing = (tile_forcing.astype(jnp.float32)[tile_of] + elevation_gap[:, None] * lapse_rate[None, :]).astype(jnp.bfloat16)
    state_in = land_state.astype(jnp.bfloat16)
    inputs = jnp.concatenate([column_forcing, state_in[column_target]], axis=1)
    blocks = inputs.reshape(COLS // A_COLS, A_COLS, FEATURES)
    result = lax.map(lambda block: network(block, w_in, norm_gains, w_up, w_down, w_out), blocks)
    result = result.reshape(COLS, STATE + FLUX)
    tendency = jnp.zeros((SLOTS, STATE), jnp.float32).at[column_target].set(result[:, :STATE].astype(jnp.float32))
    slot_index = jnp.arange(SLOTS, dtype=jnp.int32)
    living = slot_index % CAP < owner_counts[slot_index // CAP]
    new_state = jnp.where(living[:, None], land_state + tendency, jnp.float32(0.0))
    flux = result[:, STATE:].astype(jnp.float32)
    totals = jax.ops.segment_sum(flux, tile_of, TILES)
    numbers = jax.ops.segment_sum(jnp.ones((COLS,), jnp.float32), tile_of, TILES)
    tile_flux = totals / jnp.maximum(numbers, 1.0)[:, None]
    return (new_state, tile_flux)
```

```python
import functools

import jax
import jax.numpy as jnp
from jax import lax
from jax.experimental import pallas as pl
from jax.experimental.pallas import tpu as pltpu
from jax.sharding import PartitionSpec as P

F32 = jnp.float32
BF16 = jnp.bfloat16
LANES = 128
VMEM = pl.BlockSpec(memory_space=pltpu.VMEM)
SMEM = pl.BlockSpec(memory_space=pltpu.SMEM)
ANY = pl.BlockSpec(memory_space=pl.ANY)
MESH = pl.DeviceIdType.MESH


def dot(a, b):
    return jnp.dot(a, b, preferred_element_type=F32)


def dot_nt(a, b):
    return lax.dot_general(a, b, (((1,), (1,)), ((), ())), preferred_element_type=F32)


def dot_tn(a, b):
    return lax.dot_general(a, b, (((0,), (0,)), ((), ())), preferred_element_type=F32)


def iota(shape, dim):
    return lax.broadcasted_iota(jnp.int32, shape, dim)


def hot(mask):
    return jnp.where(mask, 1.0, 0.0)


def prep_kernel(
    n, per_peer, rows, capacity, tf_ref, gap_ref, lapse_ref, tile_ref, target_ref,
    send_ref, slots_ref, hots_ref, counts_ref,
):
    columns = target_ref.shape[1]
    tiles = tf_ref.shape[0]
    target = target_ref[...].astype(F32)
    owner_f = jnp.floor((target + 0.5) * (1.0 / capacity))
    slot_p = target - owner_f * capacity + 1.0
    owner = owner_f.astype(jnp.int32)
    owner_hot = hot(iota((n, columns), 0) == owner)
    owner_bf = owner_hot.astype(BF16)
    block = min(256, columns)
    upper = hot(iota((block, block), 0) <= iota((block, block), 1)).astype(BF16)
    running = jnp.zeros((n, 1), F32)
    ranks = []
    for b in range(columns // block):
        part = slice(b * block, (b + 1) * block)
        seen = dot(owner_bf[:, part], upper)
        ranks.append(jnp.sum(owner_hot[:, part] * (seen + running), axis=0, keepdims=True) - 1.0)
        running = running + seen[:, block - 1 : block]
    rank = jnp.concatenate(ranks, axis=1).astype(jnp.int32)
    place = hot(iota((LANES, columns), 0) == rank)
    high = jnp.floor(slot_p * (1.0 / 64.0))
    low = slot_p - 64.0 * high
    slot_hi = dot_nt(owner_bf, (place * high).astype(BF16))
    slot_lo = dot_nt(owner_bf, (place * low).astype(BF16))
    slot = slot_hi * 64.0 + slot_lo - 1.0
    slots_ref[...] = jnp.where(slot < 0.0, float(capacity), slot).astype(jnp.int32)
    tile = tile_ref[...]
    gap = gap_ref[...]
    gap_1 = gap.astype(BF16).astype(F32)
    gap_2 = (gap - gap_1).astype(BF16).astype(F32)
    gap_3 = gap - gap_1 - gap_2
    short = place[:rows]
    tile_of = dot_nt((short * (tile.astype(F32) + 1.0)).astype(BF16), owner_bf)
    gap_of = (
        dot_nt((short * gap_1).astype(BF16), owner_bf)
        + dot_nt((short * gap_2).astype(BF16), owner_bf)
    ) + dot_nt((short * gap_3).astype(BF16), owner_bf)
    number = jnp.sum(hot(iota((tiles, columns), 0) == tile), axis=1, keepdims=True)
    counts_ref[...] = jnp.broadcast_to(jnp.maximum(number, 1.0), counts_ref.shape)
    group = min(16, n)
    lapse = lapse_ref[...]
    table = tf_ref[...]
    lane = iota((rows, tiles), 1).astype(F32) + 1.0

    def body(b, carry):
        tile_now, gap_now = carry
        hots = jnp.concatenate(
            [hot(lane == tile_now[:, i : i + 1]).astype(BF16) for i in range(group)], axis=0
        )
        lifts = jnp.concatenate([gap_now[:, i : i + 1] * lapse for i in range(group)], axis=0)
        forcing = (dot(hots, table) + lifts).astype(BF16)
        spot = pl.ds(b * group, group)
        hots_ref[spot] = hots.reshape(group, rows, tiles)
        send_ref[spot] = forcing.reshape(group, rows, LANES)
        return (
            pltpu.roll(tile_now, n - group, axis=1) if n > group else tile_now,
            pltpu.roll(gap_now, n - group, axis=1) if n > group else gap_now,
        )

    lax.fori_loop(0, n // group, body, (tile_of, gap_of))


def net(x_ref, hid, low, act, gains, w_in, w_up, w_down, w_out, width):
    hidden = hid.shape[1]
    parts = [slice(i * width, (i + 1) * width) for i in range(hidden // width)]
    x = x_ref[...]
    total = None
    for c in parts:
        h = dot(x, w_in[:, c])
        hid[:, c] = h
        low[:, c] = (h * gains[0:1, c]).astype(BF16)
        s = jnp.sum(h * h, axis=1, keepdims=True)
        total = s if total is None else total + s
    half = lax.rsqrt(total * (1.0 / hidden) + 1e-6) * 0.5
    for c in parts:
        v = dot(low[...], w_up[:, c]) * half
        act[:, c] = (v + v * jnp.tanh(v)).astype(BF16)
    total = None
    for c in parts:
        h = hid[:, c] + dot(act[...], w_down[:, c])
        low[:, c] = (h * gains[1:2, c]).astype(BF16)
        s = jnp.sum(h * h, axis=1, keepdims=True)
        total = s if total is None else total + s
    scale = lax.rsqrt(total * (1.0 / hidden) + 1e-6)
    return dot(low[...], w_out[...]) * scale


def main_kernel(
    sizes, per_peer, rows, capacity, group, width,
    send_ref, slots_ref, land_ref, gains_ref, w_in_ref, w_up_ref, w_down_ref, w_out_ref,
    fresh_ref, got_slots, flux_ref,
    got, slots_s, land, w_in, w_up, w_down, w_out, state, forcing, x, hid, low, act, flux, back,
    load_sem, slot_send, slot_recv, send_sem, recv_sem, back_send, back_recv, smem_sem,
):
    n_atm, n_land = sizes
    n = n_atm * n_land
    atm = lax.axis_index("atm")
    lnd = lax.axis_index("land")
    me = atm * n_land + lnd
    block = group * per_peer

    def ahead(d):
        return lax.rem(atm + d // n_land, n_atm), lax.rem(lnd + lax.rem(d, n_land), n_land)

    def behind(d):
        return (
            lax.rem(atm - d // n_land + n_atm, n_atm),
            lax.rem(lnd - lax.rem(d, n_land) + n_land, n_land),
        )

    barrier = pltpu.get_barrier_semaphore()

    def greet(d, carry):
        pl.semaphore_signal(barrier, inc=1, device_id=ahead(d), device_id_type=MESH)
        return carry

    lax.fori_loop(1, n, greet, 0)
    loads = [
        pltpu.make_async_copy(src, dst, load_sem.at[i])
        for i, (src, dst) in enumerate(
            [
                (land_ref, land.at[pl.ds(0, capacity)]),
                (w_in_ref, w_in),
                (w_up_ref, w_up),
                (w_down_ref, w_down),
                (w_out_ref, w_out),
            ]
        )
    ]
    for load in loads:
        load.start()
    land[pl.ds(capacity, 8), :] = jnp.zeros((8, LANES), F32)
    flux[pl.ds(block, 8), :] = jnp.zeros((8, LANES), F32)
    got_slots[0] = slots_ref[me]
    got[0] = send_ref[me]
    pl.semaphore_wait(barrier, n - 1)

    def slot_copy(d):
        a, b = ahead(d)
        return pltpu.make_async_remote_copy(
            src_ref=slots_ref.at[a * n_land + b], dst_ref=got_slots.at[d],
            send_sem=slot_send, recv_sem=slot_recv, device_id=(a, b), device_id_type=MESH,
        )

    def forcing_copy(d):
        a, b = ahead(d)
        return pltpu.make_async_remote_copy(
            src_ref=send_ref.at[a * n_land + b], dst_ref=got.at[d],
            send_sem=send_sem, recv_sem=recv_sem.at[d // group], device_id=(a, b), device_id_type=MESH,
        )

    def start_slots(d, carry):
        slot_copy(d).start()
        return carry

    def start_forcing(d, carry):
        forcing_copy(d).start()
        return carry

    lax.fori_loop(1, n, start_slots, 0)
    lax.fori_loop(1, n, start_forcing, 0)

    def many(ref, start, count, send, recv):
        spot = ref.at[pl.ds(start, count)]
        return pltpu.make_async_remote_copy(
            src_ref=spot, dst_ref=spot, send_sem=send, recv_sem=recv,
            device_id=ahead(1), device_id_type=MESH,
        )

    many(got_slots, 1, n - 1, slot_send, slot_recv).wait_recv()
    to_smem = pltpu.make_async_copy(got_slots, slots_s, smem_sem)
    to_smem.start()
    to_smem.wait()
    for load in loads:
        load.wait()

    def chunk(g, carry):
        first = g * group

        @pl.when(g == 0)
        def _():
            many(got, 1, group - 1, send_sem, recv_sem.at[0]).wait_recv()

        @pl.when(g > 0)
        def _():
            many(got, first, group, send_sem, recv_sem.at[g]).wait_recv()

        for p in range(group):
            for k in range(per_peer):
                slot = slots_s[first + p, 0, k]
                state[pl.ds(p * per_peer + k, 1), :] = land[pl.ds(slot, 1), :]
            forcing[pl.ds(p * per_peer, per_peer), :] = got[first + p, :per_peer, :].astype(F32)
        x[:, :LANES] = forcing[...].astype(BF16)
        x[:, LANES:] = state[...].astype(BF16)
        result = net(x, hid, low, act, gains_ref, w_in, w_up, w_down, w_out, width)
        tendency = result[:, :LANES].astype(BF16).astype(F32)
        fresh_ref[pl.ds(pl.multiple_of(g * block, 8), block), :] = state[...] + tendency
        flux[pl.ds(0, block), :] = result[:, LANES:]
        for p in range(group):
            back[first + p] = flux[pl.ds(p * per_peer, rows), :].astype(BF16)

        def give(p, carry):
            d = first + p

            @pl.when(d > 0)
            def _():
                pltpu.make_async_remote_copy(
                    src_ref=back.at[d], dst_ref=flux_ref.at[me],
                    send_sem=back_send, recv_sem=back_recv, device_id=behind(d), device_id_type=MESH,
                ).start()

            return carry

        lax.fori_loop(0, group, give, 0)
        return carry

    lax.fori_loop(0, n // group, chunk, 0)
    flux_ref[me] = back[0]
    many(got_slots, 1, n - 1, slot_send, slot_recv).wait_send()
    many(got, 1, n - 1, send_sem, recv_sem.at[0]).wait_send()
    many(back, 1, n - 1, back_send, back_recv).wait_send()
    many(back, 1, n - 1, back_send, back_recv).wait_recv()


def finish_kernel(n, per_peer, capacity, slots_ref, fresh_ref, flux_ref, hots_ref, counts_ref,
                  state_ref, tile_ref, out, sem):
    def clear(i, carry):
        out[pl.ds(i * 64, 64), :] = jnp.zeros((64, LANES), F32)
        return carry

    lax.fori_loop(0, capacity // 64, clear, 0)
    if capacity % 64:
        out[pl.ds(capacity // 64 * 64, capacity % 64), :] = jnp.zeros((capacity % 64, LANES), F32)

    def place(d, carry):
        for k in range(per_peer):
            slot = slots_ref[d, 0, k]
            out[pl.ds(slot, 1), :] = fresh_ref[pl.ds(d * per_peer + k, 1), :]
        return carry

    lax.fori_loop(0, n, place, 0)
    copy = pltpu.make_async_copy(out.at[pl.ds(0, capacity)], state_ref, sem)
    copy.start()
    total = hots_ref.shape[0]
    step = total // 8
    acc = None
    for i in range(8):
        part = slice(i * step, (i + 1) * step)
        t = dot_tn(hots_ref[part, :], flux_ref[part, :])
        acc = t if acc is None else acc + t
    tile_ref[...] = acc / counts_ref[...]
    copy.wait()


def limit(mib):
    return pltpu.CompilerParams(vmem_limit_bytes=mib * 1024 * 1024)


def local(
    sizes, tile_forcing, elevation_gap, lapse_rate, column_tile, column_target, owner_counts,
    land_state, w_in, norm_gains, w_up, w_down, w_out,
):
    n = sizes[0] * sizes[1]
    capacity = land_state.shape[0]
    per_peer = capacity // n + 1
    rows = -(-per_peer // 16) * 16
    columns = elevation_gap.shape[0]
    tiles, features = tile_forcing.shape
    hidden = w_in.shape[1]
    group = 16 if n % 16 == 0 else 2
    block = group * per_peer
    S = jax.ShapeDtypeStruct
    send, slots, hots, counts = pl.pallas_call(
        functools.partial(prep_kernel, n, per_peer, rows, capacity),
        out_shape=[
            S((n, rows, features), BF16), S((n, LANES), jnp.int32),
            S((n, rows, tiles), BF16), S((tiles, features), F32),
        ],
        in_specs=[VMEM] * 5,
        out_specs=[VMEM] * 4,
        compiler_params=limit(48),
        name="prep",
    )(
        tile_forcing, elevation_gap.reshape(1, columns), lapse_rate.reshape(1, features),
        column_tile.reshape(1, columns), column_target.reshape(1, columns),
    )
    slots = slots.reshape(n, 1, LANES)
    dma = pltpu.SemaphoreType.DMA
    fresh, got_slots, flux = pl.pallas_call(
        functools.partial(main_kernel, sizes, per_peer, rows, capacity, group, 256),
        out_shape=[
            S((n * per_peer, features), F32), S((n, 1, LANES), jnp.int32), S((n, rows, features), BF16),
        ],
        in_specs=[VMEM, VMEM, ANY, VMEM, ANY, ANY, ANY, ANY],
        out_specs=[VMEM] * 3,
        scratch_shapes=[
            pltpu.VMEM((n, rows, features), BF16),
            pltpu.SMEM((n, 1, LANES), jnp.int32),
            pltpu.VMEM((capacity + 8, features), F32),
            pltpu.VMEM(w_in.shape, BF16),
            pltpu.VMEM(w_up.shape[1:], BF16),
            pltpu.VMEM(w_down.shape[1:], BF16),
            pltpu.VMEM(w_out.shape, BF16),
            pltpu.VMEM((block, features), F32),
            pltpu.VMEM((block, features), F32),
            pltpu.VMEM((block, 2 * features), BF16),
            pltpu.VMEM((block, hidden), F32),
            pltpu.VMEM((block, hidden), BF16),
            pltpu.VMEM((block, hidden), BF16),
            pltpu.VMEM((block + 8, features), F32),
            pltpu.VMEM((n, rows, features), BF16),
            dma((5,)), dma(()), dma(()), dma(()), dma((n // group,)), dma(()), dma(()), dma(()),
        ],
        compiler_params=pltpu.CompilerParams(
            collective_id=0, has_side_effects=True, vmem_limit_bytes=60 * 1024 * 1024
        ),
        name="exchange",
    )(send, slots, land_state, norm_gains, w_in, w_up[0], w_down[0], w_out)
    return pl.pallas_call(
        functools.partial(finish_kernel, n, per_peer, capacity),
        out_shape=[S((capacity, features), F32), S((tiles, features), F32)],
        in_specs=[SMEM, VMEM, VMEM, VMEM, VMEM],
        out_specs=[ANY, VMEM],
        scratch_shapes=[pltpu.VMEM((capacity + 8, features), F32), dma(())],
        compiler_params=limit(32),
        name="finish",
    )(
        got_slots, fresh, flux.reshape(n * rows, features), hots.reshape(n * rows, tiles), counts
    )


def solution(mesh):
    both = P(("atm", "land"))
    wide = P(("atm", "land"), None)
    sizes = (mesh.shape["atm"], mesh.shape["land"])
    return jax.shard_map(
        functools.partial(local, sizes),
        mesh=mesh,
        in_specs=(wide, both, P(), both, both, both, wide, P(), P(), P(), P(), P()),
        out_specs=(wide, wide),
        check_vma=False,
    )
```

```python
import functools

import jax
import jax.numpy as jnp
from jax import lax
from jax.experimental import pallas as pl
from jax.experimental.pallas import tpu as pltpu
from jax.sharding import PartitionSpec as P

F32 = jnp.float32
BF16 = jnp.bfloat16
LANES = 128
VMEM = pl.BlockSpec(memory_space=pltpu.VMEM)
HBM = pl.BlockSpec(memory_space=pltpu.HBM)
ANY = pl.BlockSpec(memory_space=pl.ANY)
MESH = pl.DeviceIdType.MESH


def dot(a, b):
    return jnp.dot(a, b, preferred_element_type=F32)


def dot_nt(a, b):
    return lax.dot_general(a, b, (((1,), (1,)), ((), ())), preferred_element_type=F32)


def dot_tn(a, b):
    return lax.dot_general(a, b, (((0,), (0,)), ((), ())), preferred_element_type=F32)


def iota(shape, dim):
    return lax.broadcasted_iota(jnp.int32, shape, dim)


def hot(mask):
    return jnp.where(mask, 1.0, 0.0)


def prepare(
    n, per_peer, rows, capacity, tf_ref, gap_ref, lapse_ref, tile_ref, target_ref,
    send_ref, slots_ref, hots_ref, counts_ref,
):
    columns = target_ref.shape[1]
    tiles = tf_ref.shape[0]
    target = target_ref[...].astype(F32)
    owner_f = jnp.floor((target + 0.5) * (1.0 / capacity))
    slot_p = target - owner_f * capacity + 1.0
    owner = owner_f.astype(jnp.int32)
    owner_hot = hot(iota((n, columns), 0) == owner)
    owner_bf = owner_hot.astype(BF16)
    block = min(256, columns)
    upper = hot(iota((block, block), 0) <= iota((block, block), 1)).astype(BF16)
    running = jnp.zeros((n, 1), F32)
    ranks = []
    for b in range(columns // block):
        part = slice(b * block, (b + 1) * block)
        seen = dot(owner_bf[:, part], upper)
        ranks.append(jnp.sum(owner_hot[:, part] * (seen + running), axis=0, keepdims=True) - 1.0)
        running = running + seen[:, block - 1 : block]
    rank = jnp.concatenate(ranks, axis=1).astype(jnp.int32)
    place = hot(iota((LANES, columns), 0) == rank)
    high = jnp.floor(slot_p * (1.0 / 64.0))
    low = slot_p - 64.0 * high
    slot_hi = dot_nt(owner_bf, (place * high).astype(BF16))
    slot_lo = dot_nt(owner_bf, (place * low).astype(BF16))
    slot = slot_hi * 64.0 + slot_lo - 1.0
    slot = jnp.where(slot < 0.0, float(capacity), slot).astype(jnp.int32)
    for j in range(n):
        slots_ref[j] = slot[j : j + 1, :]
    tile = tile_ref[...]
    gap = gap_ref[...]
    gap_1 = gap.astype(BF16).astype(F32)
    gap_2 = (gap - gap_1).astype(BF16).astype(F32)
    gap_3 = gap - gap_1 - gap_2
    short = place[:rows]
    tile_of = dot_nt((short * (tile.astype(F32) + 1.0)).astype(BF16), owner_bf)
    gap_of = (
        dot_nt((short * gap_1).astype(BF16), owner_bf)
        + dot_nt((short * gap_2).astype(BF16), owner_bf)
    ) + dot_nt((short * gap_3).astype(BF16), owner_bf)
    number = jnp.sum(hot(iota((tiles, columns), 0) == tile), axis=1, keepdims=True)
    counts_ref[...] = jnp.broadcast_to(jnp.maximum(number, 1.0), counts_ref.shape)
    group = min(16, n)
    lapse = lapse_ref[...]
    table = tf_ref[...]
    lane = iota((rows, tiles), 1).astype(F32) + 1.0

    def body(b, carry):
        tile_now, gap_now = carry
        hots = jnp.concatenate(
            [hot(lane == tile_now[:, i : i + 1]).astype(BF16) for i in range(group)], axis=0
        )
        lifts = jnp.concatenate([gap_now[:, i : i + 1] * lapse for i in range(group)], axis=0)
        forcing = (dot(hots, table) + lifts).astype(BF16)
        spot = pl.ds(b * group, group)
        hots_ref[spot] = hots.reshape(group, rows, tiles)
        send_ref[spot] = forcing.reshape(group, rows, LANES)
        return (
            pltpu.roll(tile_now, n - group, axis=1) if n > group else tile_now,
            pltpu.roll(gap_now, n - group, axis=1) if n > group else gap_now,
        )

    lax.fori_loop(0, n // group, body, (tile_of, gap_of))


def net(x_ref, hid, low, act, gains, w_in, w_up, w_down, w_out, width, fill):
    hidden = hid.shape[1]
    parts = [slice(i * width, (i + 1) * width) for i in range(hidden // width)]
    x = x_ref[...]
    total = None
    for c in parts:
        h = dot(x, w_in[:, c])
        hid[:, c] = h
        low[:, c] = (h * gains[0:1, c]).astype(BF16)
        s = jnp.sum(h * h, axis=1, keepdims=True)
        total = s if total is None else total + s
        fill()
    half = lax.rsqrt(total * (1.0 / hidden) + 1e-6) * 0.5
    for c in parts:
        v = dot(low[...], w_up[:, c]) * half
        act[:, c] = (v + v * jnp.tanh(v)).astype(BF16)
        fill()
    total = None
    for c in parts:
        h = hid[:, c] + dot(act[...], w_down[:, c])
        low[:, c] = (h * gains[1:2, c]).astype(BF16)
        s = jnp.sum(h * h, axis=1, keepdims=True)
        total = s if total is None else total + s
        fill()
    scale = lax.rsqrt(total * (1.0 / hidden) + 1e-6)
    return dot(low[...], w_out[...]) * scale


def main_kernel(
    sizes, per_peer, rows, capacity, group, width,
    tf_hbm, gap_hbm, lapse_hbm, tile_hbm, target_hbm,
    land_hbm, gains_hbm, w_in_hbm, w_up_hbm, w_down_hbm, w_out_hbm,
    fresh_ref, got_slots, flux_ref, hots_ref, counts_ref,
    tf, gap, lapse, tile, target, land, gains, w_in, w_up, w_down, w_out,
    send, slots, got, slots_s, ahead_state, state, forcing, x, hid, low, act, flux, back,
    load_sem, slot_send, slot_recv, send_sem, recv_sem, back_send, back_recv, smem_sem,
):
    n_atm, n_land = sizes
    n = n_atm * n_land
    atm = lax.axis_index("atm")
    lnd = lax.axis_index("land")
    me = atm * n_land + lnd
    block = group * per_peer

    def ahead(d):
        return lax.rem(atm + d // n_land, n_atm), lax.rem(lnd + lax.rem(d, n_land), n_land)

    def behind(d):
        return (
            lax.rem(atm - d // n_land + n_atm, n_atm),
            lax.rem(lnd - lax.rem(d, n_land) + n_land, n_land),
        )

    barrier = pltpu.get_barrier_semaphore()

    def greet(d, carry):
        pl.semaphore_signal(barrier, inc=1, device_id=ahead(d), device_id_type=MESH)
        return carry

    lax.fori_loop(1, n, greet, 0)
    loads = [
        pltpu.make_async_copy(src, dst, load_sem.at[i])
        for i, (src, dst) in enumerate(
            [
                (target_hbm, target),
                (tile_hbm, tile),
                (gap_hbm, gap),
                (lapse_hbm, lapse),
                (tf_hbm, tf),
                (land_hbm, land.at[pl.ds(0, capacity)]),
                (gains_hbm, gains),
                (w_in_hbm, w_in),
                (w_up_hbm, w_up),
                (w_down_hbm, w_down),
                (w_out_hbm, w_out),
            ]
        )
    ]
    for load in loads:
        load.start()
    land[pl.ds(capacity, 8), :] = jnp.zeros((8, LANES), F32)
    flux[pl.ds(block, 8), :] = jnp.zeros((8, LANES), F32)
    for load in loads[:5]:
        load.wait()
    prepare(
        n, per_peer, rows, capacity, tf, gap, lapse, tile, target, send, slots, hots_ref, counts_ref
    )
    got_slots[0] = slots[me]
    got[0] = send[me]
    pl.semaphore_wait(barrier, n - 1)

    def slot_copy(d):
        a, b = ahead(d)
        return pltpu.make_async_remote_copy(
            src_ref=slots.at[a * n_land + b], dst_ref=got_slots.at[d],
            send_sem=slot_send, recv_sem=slot_recv, device_id=(a, b), device_id_type=MESH,
        )

    def forcing_copy(d):
        a, b = ahead(d)
        return pltpu.make_async_remote_copy(
            src_ref=send.at[a * n_land + b], dst_ref=got.at[d],
            send_sem=send_sem, recv_sem=recv_sem.at[d // group], device_id=(a, b), device_id_type=MESH,
        )

    def start_slots(d, carry):
        slot_copy(d).start()
        return carry

    def start_forcing(d, carry):
        forcing_copy(d).start()
        return carry

    lax.fori_loop(1, n, start_slots, 0)
    lax.fori_loop(1, n, start_forcing, 0)

    def many(ref, start, count, send, recv):
        spot = ref.at[pl.ds(start, count)]
        return pltpu.make_async_remote_copy(
            src_ref=spot, dst_ref=spot, send_sem=send, recv_sem=recv,
            device_id=ahead(1), device_id_type=MESH,
        )

    many(got_slots, 1, n - 1, slot_send, slot_recv).wait_recv()
    to_smem = pltpu.make_async_copy(got_slots, slots_s, smem_sem)
    to_smem.start()
    to_smem.wait()
    for load in loads[5:]:
        load.wait()

    def fetch(peer, p, k):
        slot = jnp.clip(slots_s[peer, 0, k], 0, capacity)
        ahead_state[pl.ds(p * per_peer + k, 1), :] = land[pl.ds(slot, 1), :]

    def fetch_all(p, carry):
        for k in range(per_peer):
            fetch(p, p, k)
        return carry

    lax.fori_loop(0, group, fetch_all, 0)

    def chunk(g, carry):
        first = g * group

        @pl.when(g == 0)
        def _():
            many(got, 1, group - 1, send_sem, recv_sem.at[0]).wait_recv()

        @pl.when(g > 0)
        def _():
            many(got, first, group, send_sem, recv_sem.at[g]).wait_recv()

        for p in range(group):
            forcing[pl.ds(p * per_peer, per_peer), :] = got[first + p, :per_peer, :].astype(F32)
        x[:, :LANES] = forcing[...].astype(BF16)
        now = ahead_state[...]
        state[...] = now
        x[:, LANES:] = now.astype(BF16)
        following = jnp.minimum(first + group, n - group)
        todo = [(p, k) for p in range(group) for k in range(per_peer)]
        share = -(-len(todo) // (3 * (hid.shape[1] // width)))

        def fill():
            for p, k in todo[:share]:
                fetch(following + p, p, k)
            del todo[:share]

        result = net(x, hid, low, act, gains, w_in, w_up, w_down, w_out, width, fill)
        tendency = result[:, :LANES].astype(BF16).astype(F32)
        fresh_ref[pl.ds(pl.multiple_of(g * block, 8), block), :] = state[...] + tendency
        flux[pl.ds(0, block), :] = result[:, LANES:]
        for p in range(group):
            back[first + p] = flux[pl.ds(p * per_peer, rows), :].astype(BF16)

        def give(p, carry):
            d = first + p

            @pl.when(d > 0)
            def _():
                pltpu.make_async_remote_copy(
                    src_ref=back.at[d], dst_ref=flux_ref.at[me],
                    send_sem=back_send, recv_sem=back_recv, device_id=behind(d), device_id_type=MESH,
                ).start()

            return carry

        lax.fori_loop(0, group, give, 0)
        return carry

    lax.fori_loop(0, n // group, chunk, 0)
    flux_ref[me] = back[0]
    many(got_slots, 1, n - 1, slot_send, slot_recv).wait_send()
    many(got, 1, n - 1, send_sem, recv_sem.at[0]).wait_send()
    many(back, 1, n - 1, back_send, back_recv).wait_send()
    many(back, 1, n - 1, back_send, back_recv).wait_recv()


def finish_kernel(n, per_peer, capacity, slots_hbm, fresh_ref, flux_ref, hots_ref, counts_ref,
                  state_ref, tile_ref, out, slots_ref, sem, smem_sem):
    to_smem = pltpu.make_async_copy(slots_hbm, slots_ref, smem_sem)
    to_smem.start()
    total = hots_ref.shape[0]
    step = total // 8
    acc = None
    for i in range(8):
        part = slice(i * step, (i + 1) * step)
        t = dot_tn(hots_ref[part, :], flux_ref[part, :])
        acc = t if acc is None else acc + t
    tile_ref[...] = acc / counts_ref[...]

    def clear(i, carry):
        out[pl.ds(i * 64, 64), :] = jnp.zeros((64, LANES), F32)
        return carry

    lax.fori_loop(0, capacity // 64, clear, 0)
    if capacity % 64:
        out[pl.ds(capacity // 64 * 64, capacity % 64), :] = jnp.zeros((capacity % 64, LANES), F32)

    def place(d, carry):
        for k in range(per_peer):
            slot = slots_ref[d, 0, k]
            out[pl.ds(slot, 1), :] = fresh_ref[pl.ds(d * per_peer + k, 1), :]
        return carry

    to_smem.wait()
    lax.fori_loop(0, n, place, 0)
    copy = pltpu.make_async_copy(out.at[pl.ds(0, capacity)], state_ref, sem)
    copy.start()
    copy.wait()


def limit(mib):
    return pltpu.CompilerParams(vmem_limit_bytes=mib * 1024 * 1024)


def local(
    sizes, tile_forcing, elevation_gap, lapse_rate, column_tile, column_target, owner_counts,
    land_state, w_in, norm_gains, w_up, w_down, w_out,
):
    n = sizes[0] * sizes[1]
    capacity = land_state.shape[0]
    per_peer = capacity // n + 1
    rows = -(-per_peer // 16) * 16
    columns = elevation_gap.shape[0]
    tiles, features = tile_forcing.shape
    hidden = w_in.shape[1]
    group = 16 if n % 16 == 0 else 2
    block = group * per_peer
    S = jax.ShapeDtypeStruct
    dma = pltpu.SemaphoreType.DMA
    fresh, got_slots, flux, hots, counts = pl.pallas_call(
        functools.partial(main_kernel, sizes, per_peer, rows, capacity, group, 256),
        out_shape=[
            S((n * per_peer, features), F32), S((n, 1, LANES), jnp.int32), S((n, rows, features), BF16),
            S((n, rows, tiles), BF16), S((tiles, features), F32),
        ],
        in_specs=[HBM] * 11,
        out_specs=[VMEM] * 5,
        scratch_shapes=[
            pltpu.VMEM((tiles, features), BF16),
            pltpu.VMEM((1, columns), F32),
            pltpu.VMEM((1, features), F32),
            pltpu.VMEM((1, columns), jnp.int32),
            pltpu.VMEM((1, columns), jnp.int32),
            pltpu.VMEM((capacity + 8, features), F32),
            pltpu.VMEM(norm_gains.shape, F32),
            pltpu.VMEM(w_in.shape, BF16),
            pltpu.VMEM(w_up.shape[1:], BF16),
            pltpu.VMEM(w_down.shape[1:], BF16),
            pltpu.VMEM(w_out.shape, BF16),
            pltpu.VMEM((n, rows, features), BF16),
            pltpu.VMEM((n, 1, LANES), jnp.int32),
            pltpu.VMEM((n, rows, features), BF16),
            pltpu.SMEM((n, 1, LANES), jnp.int32),
            pltpu.VMEM((block, features), F32),
            pltpu.VMEM((block, features), F32),
            pltpu.VMEM((block, features), F32),
            pltpu.VMEM((block, 2 * features), BF16),
            pltpu.VMEM((block, hidden), F32),
            pltpu.VMEM((block, hidden), BF16),
            pltpu.VMEM((block, hidden), BF16),
            pltpu.VMEM((block + 8, features), F32),
            pltpu.VMEM((n, rows, features), BF16),
            dma((11,)), dma(()), dma(()), dma(()), dma((n // group,)), dma(()), dma(()), dma(()),
        ],
        compiler_params=pltpu.CompilerParams(
            collective_id=0, has_side_effects=True, vmem_limit_bytes=40 * 1024 * 1024
        ),
        name="exchange",
    )(
        *[
            pltpu.with_memory_space_constraint(v, pltpu.HBM)
            for v in (
                tile_forcing, elevation_gap.reshape(1, columns), lapse_rate.reshape(1, features),
                column_tile.reshape(1, columns), column_target.reshape(1, columns),
                land_state, norm_gains, w_in, w_up[0], w_down[0], w_out,
            )
        ]
    )
    return pl.pallas_call(
        functools.partial(finish_kernel, n, per_peer, capacity),
        out_shape=[S((capacity, features), F32), S((tiles, features), F32)],
        in_specs=[VMEM] * 5,
        out_specs=[ANY, VMEM],
        scratch_shapes=[
            pltpu.VMEM((capacity + 8, features), F32), pltpu.SMEM((n, 1, LANES), jnp.int32),
            dma(()), dma(()),
        ],
        compiler_params=limit(24),
        name="finish",
    )(
        got_slots, fresh, flux.reshape(n * rows, features), hots.reshape(n * rows, tiles), counts
    )


def solution(mesh):
    both = P(("atm", "land"))
    wide = P(("atm", "land"), None)
    sizes = (mesh.shape["atm"], mesh.shape["land"])
    return jax.shard_map(
        functools.partial(local, sizes),
        mesh=mesh,
        in_specs=(wide, both, P(), both, both, both, wide, P(), P(), P(), P(), P()),
        out_specs=(wide, wide),
        check_vma=False,
    )
```

```python
import functools

import jax
import jax.numpy as jnp
from jax import lax
from jax.experimental import pallas as pl
from jax.experimental.pallas import tpu as pltpu
from jax.sharding import PartitionSpec as P

F32 = jnp.float32
BF16 = jnp.bfloat16
LANES = 128
HALF = 64
VMEM = pl.BlockSpec(memory_space=pltpu.VMEM)
HBM = pl.BlockSpec(memory_space=pltpu.HBM)
ANY = pl.BlockSpec(memory_space=pl.ANY)
MESH = pl.DeviceIdType.MESH


def dot(a, b):
    return jnp.dot(a, b, preferred_element_type=F32)


def dot_nt(a, b):
    return lax.dot_general(a, b, (((1,), (1,)), ((), ())), preferred_element_type=F32)


def dot_tn(a, b):
    return lax.dot_general(a, b, (((0,), (0,)), ((), ())), preferred_element_type=F32)


def iota(shape, dim):
    return lax.broadcasted_iota(jnp.int32, shape, dim)


def hot(mask):
    return jnp.where(mask, 1.0, 0.0)


def tables(sizes, atm, lnd, per_peer, rows, capacity, gap_ref, tile_ref, target_ref, counts_ref):
    n_atm, n_land = sizes
    n = n_atm * n_land
    columns = target_ref.shape[1]
    tiles = counts_ref.shape[0]
    target = target_ref[...].astype(F32)
    owner_f = jnp.floor((target + 0.5) * (1.0 / capacity))
    slot_p = target - owner_f * capacity + 1.0
    owner_atm = jnp.floor((owner_f + 0.5) * (1.0 / n_land))
    owner_land = owner_f - owner_atm * n_land
    step = owner_land - lnd.astype(F32)
    step = jnp.where(step < 0.0, step + n_land, step)
    turn = owner_atm - atm.astype(F32) - step + (n_land + n_atm)
    turn = turn - jnp.floor((turn + 0.5) * (1.0 / n_atm)) * n_atm
    order = (turn * n_land + step).astype(jnp.int32)
    owner_hot = hot(iota((n, columns), 0) == order)
    owner_bf = owner_hot.astype(BF16)
    block = min(256, columns)
    upper = hot(iota((block, block), 0) <= iota((block, block), 1)).astype(BF16)
    running = jnp.zeros((n, 1), F32)
    ranks = []
    for b in range(columns // block):
        part = slice(b * block, (b + 1) * block)
        seen = dot(owner_bf[:, part], upper)
        ranks.append(jnp.sum(owner_hot[:, part] * (seen + running), axis=0, keepdims=True) - 1.0)
        running = running + seen[:, block - 1 : block]
    rank = jnp.concatenate(ranks, axis=1).astype(jnp.int32)
    place = hot(iota((HALF, columns), 0) == rank)
    high = jnp.floor(slot_p * (1.0 / 64.0))
    low = slot_p - 64.0 * high
    both = jnp.concatenate([(place * high).astype(BF16), (place * low).astype(BF16)], axis=0)
    slot_rows = dot_nt(owner_bf, both)
    tile = tile_ref[...]
    gap = gap_ref[...]
    gap_1 = gap.astype(BF16).astype(F32)
    gap_2 = (gap - gap_1).astype(BF16).astype(F32)
    gap_3 = gap - gap_1 - gap_2
    short = place[:rows]
    tile_of = dot_nt((short * (tile.astype(F32) + 1.0)).astype(BF16), owner_bf)
    gap_of = (
        dot_nt((short * gap_1).astype(BF16), owner_bf)
        + dot_nt((short * gap_2).astype(BF16), owner_bf)
    ) + dot_nt((short * gap_3).astype(BF16), owner_bf)
    number = jnp.sum(hot(iota((tiles, columns), 0) == tile), axis=1, keepdims=True)
    counts_ref[...] = jnp.broadcast_to(jnp.maximum(number, 1.0), counts_ref.shape)
    return slot_rows, tile_of, gap_of


def net(x_ref, hid, low, act, gains, w_in, w_up, w_down, w_out, width, fill):
    hidden = hid.shape[1]
    parts = [slice(i * width, (i + 1) * width) for i in range(hidden // width)]
    x = x_ref[...]
    total = None
    for c in parts:
        h = dot(x, w_in[:, c])
        hid[:, c] = h
        low[:, c] = (h * gains[0:1, c]).astype(BF16)
        s = jnp.sum(h * h, axis=1, keepdims=True)
        total = s if total is None else total + s
        fill()
    half = lax.rsqrt(total * (1.0 / hidden) + 1e-6) * 0.5
    for c in parts:
        v = dot(low[...], w_up[:, c]) * half
        act[:, c] = (v + v * jnp.tanh(v)).astype(BF16)
        fill()
    total = None
    for c in parts:
        h = hid[:, c] + dot(act[...], w_down[:, c])
        low[:, c] = (h * gains[1:2, c]).astype(BF16)
        s = jnp.sum(h * h, axis=1, keepdims=True)
        total = s if total is None else total + s
        fill()
    scale = lax.rsqrt(total * (1.0 / hidden) + 1e-6)
    return dot(low[...], w_out[...]) * scale


def main_kernel(
    sizes, per_peer, rows, capacity, width,
    tf_hbm, gap_hbm, lapse_hbm, tile_hbm, target_hbm,
    land_hbm, gains_hbm, w_in_hbm, w_up_hbm, w_down_hbm, w_out_hbm,
    fresh_ref, got_slots, flux_ref, hots_ref, counts_ref,
    tf, gap, lapse, tile, target, land, gains, w_in, w_up, w_down, w_out,
    send, slot_rows, tile_of, gap_of, got, slots_s, ahead_state, state, forcing, x, hid, low, act,
    flux, back, load_sem, send_sem, recv_sem, back_send, back_recv, smem_sem,
):
    n_atm, n_land = sizes
    n = n_atm * n_land
    group = n_land
    tiles = tf.shape[0]
    atm = lax.axis_index("atm")
    lnd = lax.axis_index("land")
    block = group * per_peer
    last = n_atm - 1
    message = pl.ds(0, -(-(per_peer + 1) // 2) * 2)

    def atm_ahead(g, p):
        return lax.rem(atm + g + p, n_atm)

    def atm_behind(g, p):
        return lax.rem(atm - g - p + n_atm + n_land + n_atm, n_atm)

    lands_ahead = [lax.rem(lnd + p, n_land) for p in range(n_land)]
    lands_behind = [lax.rem(lnd - p + n_land, n_land) for p in range(n_land)]

    barrier = pltpu.get_barrier_semaphore()

    def greet(g, carry):
        for p in range(group):
            def hello():
                pl.semaphore_signal(
                    barrier, inc=1, device_id=(atm_ahead(g, p), lands_ahead[p]), device_id_type=MESH
                )

            if p == 0:
                pl.when(g > 0)(hello)
            else:
                hello()
        return carry

    loads = [
        pltpu.make_async_copy(src, dst, load_sem.at[i])
        for i, (src, dst) in enumerate(
            [
                (target_hbm, target),
                (tile_hbm, tile),
                (gap_hbm, gap),
                (lapse_hbm, lapse),
                (tf_hbm, tf),
                (land_hbm, land.at[pl.ds(0, capacity)]),
                (gains_hbm, gains),
                (w_in_hbm, w_in),
                (w_up_hbm, w_up),
                (w_down_hbm, w_down),
                (w_out_hbm, w_out),
            ]
        )
    ]
    for load in loads:
        load.start()
    spare = rows - 16
    flux_ref[:, spare:, :] = jnp.zeros((n, 16, LANES), BF16)
    lax.fori_loop(0, n_atm, greet, 0)
    land[pl.ds(capacity, 8), :] = jnp.zeros((8, LANES), F32)
    flux[pl.ds(block, 8), :] = jnp.zeros((8, LANES), F32)
    for load in loads[:5]:
        load.wait()
    slot_rows[...], tile_of[...], gap_of[...] = tables(
        sizes, atm, lnd, per_peer, rows, capacity, gap, tile, target, counts_ref
    )
    lane = iota((rows, tiles), 1).astype(F32) + 1.0
    last_row = hot(iota((rows, LANES), 0) == per_peer)

    def build(g):
        base = g * group
        turn = lax.rem(n - base, n)
        tile_now = pltpu.roll(tile_of[...], turn, axis=1)
        gap_now = pltpu.roll(gap_of[...], turn, axis=1)
        slot_now = slot_rows[pl.ds(pl.multiple_of(base, group), group), :]
        hots = jnp.concatenate(
            [hot(lane == tile_now[:, i : i + 1]).astype(BF16) for i in range(group)], axis=0
        )
        extra = jnp.concatenate(
            [
                gap_now[:, i : i + 1] * lapse[...] + last_row * slot_now[i : i + 1, :]
                for i in range(group)
            ],
            axis=0,
        )
        made = (dot(hots, tf[...]) + extra).astype(BF16)
        spot = pl.ds(base, group)
        hots_ref[spot] = hots.reshape(group, rows, tiles)
        send[spot] = made.reshape(group, rows, LANES)

    def dispatch(g):
        for p in range(group):
            def go():
                pltpu.make_async_remote_copy(
                    src_ref=send.at[g * group + p, message],
                    dst_ref=got.at[g * group + p, message],
                    send_sem=send_sem, recv_sem=recv_sem.at[g],
                    device_id=(atm_ahead(g, p), lands_ahead[p]), device_id_type=MESH,
                ).start()

            if p == 0:
                pl.when(g > 0)(go)
            else:
                go()

    build(0)
    got[0] = send[0]
    pl.semaphore_wait(barrier, n - 1)

    def build_and_send(g, carry):
        build(g)
        dispatch(g - 1)
        return carry

    lax.fori_loop(1, n_atm, build_and_send, 0)
    dispatch(last)

    def many(ref, start, count, sending, receiving):
        spot = ref.at[pl.ds(start, count), message]
        return pltpu.make_async_remote_copy(
            src_ref=spot, dst_ref=spot, send_sem=sending, recv_sem=receiving,
            device_id=(atm, lands_ahead[1]), device_id_type=MESH,
        )

    def to_smem(g):
        spot = pl.ds(g * group, group)
        return pltpu.make_async_copy(got_slots.at[spot], slots_s.at[spot], smem_sem.at[lax.rem(g, 2)])

    base_row = per_peer // 16 * 16

    def decode(g):
        for p in range(group):
            tail = got[g * group + p, pl.ds(base_row, 16), :].astype(F32)
            row = tail[per_peer - base_row : per_peer - base_row + 1, :]
            slot = row * 64.0 + pltpu.roll(row, HALF, axis=1) - 1.0
            got_slots[g * group + p] = jnp.where(slot < 0.0, float(capacity), slot).astype(jnp.int32)
        to_smem(g).start()

    def fetch(peer, p, k):
        slot = jnp.clip(slots_s[peer, 0, k], 0, capacity)
        ahead_state[pl.ds(p * per_peer + k, 1), :] = land[pl.ds(slot, 1), :]

    def fetch_all(p, carry):
        for k in range(per_peer):
            fetch(p, p, k)
        return carry

    many(got, 1, group - 1, send_sem, recv_sem.at[0]).wait_recv()
    decode(0)
    for load in loads[5:]:
        load.wait()
    to_smem(0).wait()
    lax.fori_loop(0, group, fetch_all, 0)
    if last > 0:
        many(got, group, group, send_sem, recv_sem.at[1]).wait_recv()
        decode(1)

    def chunk(g, carry):
        first = g * group

        @pl.when(g < last - 1)
        def _():
            many(got, first + 2 * group, group, send_sem, recv_sem.at[g + 2]).wait_recv()
            decode(g + 2)

        @pl.when(g < last)
        def _():
            to_smem(g + 1).wait()

        for p in range(group):
            forcing[pl.ds(p * per_peer, per_peer), :] = got[first + p, :per_peer, :].astype(F32)
        x[:, :LANES] = forcing[...].astype(BF16)
        now = ahead_state[...]
        state[...] = now
        x[:, LANES:] = now.astype(BF16)
        following = jnp.minimum(first + group, n - group)
        todo = [(p, k) for p in range(group) for k in range(per_peer)]
        share = -(-len(todo) // (3 * (hid.shape[1] // width)))

        def fill():
            for p, k in todo[:share]:
                fetch(following + p, p, k)
            del todo[:share]

        result = net(x, hid, low, act, gains, w_in, w_up, w_down, w_out, width, fill)
        tendency = result[:, :LANES].astype(BF16).astype(F32)
        fresh_ref[pl.ds(pl.multiple_of(g * block, 8), block), :] = state[...] + tendency
        flux[pl.ds(0, block), :] = result[:, LANES:]
        for p in range(group):
            back[first + p] = flux[pl.ds(p * per_peer, rows), :].astype(BF16)
        for p in range(group):
            def give():
                a = atm_behind(g, p)
                pltpu.make_async_remote_copy(
                    src_ref=back.at[first + p, message], dst_ref=flux_ref.at[first + p, message],
                    send_sem=back_send, recv_sem=back_recv,
                    device_id=(a, lands_behind[p]), device_id_type=MESH,
                ).start()

            if p == 0:
                pl.when(g > 0)(give)
            else:
                give()
        return carry

    lax.fori_loop(0, n_atm, chunk, 0)
    flux_ref[0] = back[0]
    many(got, 1, n - 1, send_sem, recv_sem.at[0]).wait_send()
    many(back, 1, n - 1, back_send, back_recv).wait_send()
    many(back, 1, n - 1, back_send, back_recv).wait_recv()


def finish_kernel(n, per_peer, capacity, slots_hbm, fresh_ref, flux_ref, hots_ref, counts_ref,
                  state_ref, tile_ref, out, slots_ref, sem, smem_sem):
    parts = 4
    span = n // parts
    copies = [
        pltpu.make_async_copy(
            slots_hbm.at[pl.ds(i * span, span)], slots_ref.at[pl.ds(i * span, span)], smem_sem.at[i]
        )
        for i in range(parts)
    ]
    for copy in copies:
        copy.start()
    total = hots_ref.shape[0]
    step = total // 8
    acc = None
    for i in range(8):
        part = slice(i * step, (i + 1) * step)
        t = dot_tn(hots_ref[part, :], flux_ref[part, :])
        acc = t if acc is None else acc + t
    tile_ref[...] = acc / counts_ref[...]

    def clear(i, carry):
        out[pl.ds(i * 64, 64), :] = jnp.zeros((64, LANES), F32)
        return carry

    lax.fori_loop(0, capacity // 64, clear, 0)
    if capacity % 64:
        out[pl.ds(capacity // 64 * 64, capacity % 64), :] = jnp.zeros((capacity % 64, LANES), F32)

    def place(d, carry):
        for k in range(per_peer):
            slot = slots_ref[d, 0, k]
            out[pl.ds(slot, 1), :] = fresh_ref[pl.ds(d * per_peer + k, 1), :]
        return carry

    for i in range(parts):
        copies[i].wait()
        lax.fori_loop(i * span, (i + 1) * span, place, 0)
    copy = pltpu.make_async_copy(out.at[pl.ds(0, capacity)], state_ref, sem)
    copy.start()
    copy.wait()


def limit(mib):
    return pltpu.CompilerParams(vmem_limit_bytes=mib * 1024 * 1024)


def local(
    sizes, tile_forcing, elevation_gap, lapse_rate, column_tile, column_target, owner_counts,
    land_state, w_in, norm_gains, w_up, w_down, w_out,
):
    n = sizes[0] * sizes[1]
    capacity = land_state.shape[0]
    per_peer = capacity // n + 1
    rows = -(-per_peer // 16) * 16
    columns = elevation_gap.shape[0]
    tiles, features = tile_forcing.shape
    hidden = w_in.shape[1]
    group = sizes[1]
    block = group * per_peer
    S = jax.ShapeDtypeStruct
    dma = pltpu.SemaphoreType.DMA
    fresh, got_slots, flux, hots, counts = pl.pallas_call(
        functools.partial(main_kernel, sizes, per_peer, rows, capacity, 256),
        out_shape=[
            S((n * per_peer, features), F32), S((n, 1, LANES), jnp.int32), S((n, rows, features), BF16),
            S((n, rows, tiles), BF16), S((tiles, features), F32),
        ],
        in_specs=[HBM] * 11,
        out_specs=[VMEM] * 5,
        scratch_shapes=[
            pltpu.VMEM((tiles, features), BF16),
            pltpu.VMEM((1, columns), F32),
            pltpu.VMEM((1, features), F32),
            pltpu.VMEM((1, columns), jnp.int32),
            pltpu.VMEM((1, columns), jnp.int32),
            pltpu.VMEM((capacity + 8, features), F32),
            pltpu.VMEM(norm_gains.shape, F32),
            pltpu.VMEM(w_in.shape, BF16),
            pltpu.VMEM(w_up.shape[1:], BF16),
            pltpu.VMEM(w_down.shape[1:], BF16),
            pltpu.VMEM(w_out.shape, BF16),
            pltpu.VMEM((n, rows, features), BF16),
            pltpu.VMEM((n, LANES), F32),
            pltpu.VMEM((rows, n), F32),
            pltpu.VMEM((rows, n), F32),
            pltpu.VMEM((n, rows, features), BF16),
            pltpu.SMEM((n, 1, LANES), jnp.int32),
            pltpu.VMEM((block, features), F32),
            pltpu.VMEM((block, features), F32),
            pltpu.VMEM((block, features), F32),
            pltpu.VMEM((block, 2 * features), BF16),
            pltpu.VMEM((block, hidden), F32),
            pltpu.VMEM((block, hidden), BF16),
            pltpu.VMEM((block, hidden), BF16),
            pltpu.VMEM((block + 8, features), F32),
            pltpu.VMEM((n, rows, features), BF16),
            dma((11,)), dma(()), dma((n // group,)), dma(()), dma(()), dma((2,)),
        ],
        compiler_params=pltpu.CompilerParams(
            collective_id=0, has_side_effects=True, vmem_limit_bytes=40 * 1024 * 1024
        ),
        name="exchange",
    )(
        *[
            pltpu.with_memory_space_constraint(v, pltpu.HBM)
            for v in (
                tile_forcing, elevation_gap.reshape(1, columns), lapse_rate.reshape(1, features),
                column_tile.reshape(1, columns), column_target.reshape(1, columns),
                land_state, norm_gains, w_in, w_up[0], w_down[0], w_out,
            )
        ]
    )
    return pl.pallas_call(
        functools.partial(finish_kernel, n, per_peer, capacity),
        out_shape=[S((capacity, features), F32), S((tiles, features), F32)],
        in_specs=[VMEM] * 5,
        out_specs=[ANY, VMEM],
        scratch_shapes=[
            pltpu.VMEM((capacity + 8, features), F32), pltpu.SMEM((n, 1, LANES), jnp.int32),
            dma(()), dma((4,)),
        ],
        compiler_params=limit(24),
        name="finish",
    )(
        got_slots, fresh, flux.reshape(n * rows, features), hots.reshape(n * rows, tiles), counts
    )


def solution(mesh):
    both = P(("atm", "land"))
    wide = P(("atm", "land"), None)
    sizes = (mesh.shape["atm"], mesh.shape["land"])
    return jax.shard_map(
        functools.partial(local, sizes),
        mesh=mesh,
        in_specs=(wide, both, P(), both, both, both, wide, P(), P(), P(), P(), P()),
        out_specs=(wide, wide),
        check_vma=False,
    )
```

```python
import functools

import jax
import jax.numpy as jnp
from jax import lax
from jax.experimental import pallas as pl
from jax.experimental.pallas import tpu as pltpu
from jax.sharding import PartitionSpec as P

F32 = jnp.float32
BF16 = jnp.bfloat16
LANES = 128
HALF = 64
VMEM = pl.BlockSpec(memory_space=pltpu.VMEM)
HBM = pl.BlockSpec(memory_space=pltpu.HBM)
ANY = pl.BlockSpec(memory_space=pl.ANY)
MESH = pl.DeviceIdType.MESH


def dot(a, b):
    return jnp.dot(a, b, preferred_element_type=F32)


def dot_nt(a, b):
    return lax.dot_general(a, b, (((1,), (1,)), ((), ())), preferred_element_type=F32)


def dot_tn(a, b):
    return lax.dot_general(a, b, (((0,), (0,)), ((), ())), preferred_element_type=F32)


def iota(shape, dim):
    return lax.broadcasted_iota(jnp.int32, shape, dim)


def hot(mask):
    return jnp.where(mask, 1.0, 0.0)


def tables(sizes, atm, lnd, per_peer, rows, capacity, gap_ref, tile_ref, target_ref):
    n_atm, n_land = sizes
    n = n_atm * n_land
    columns = target_ref.shape[1]
    target = target_ref[...].astype(F32)
    owner_f = jnp.floor((target + 0.5) * (1.0 / capacity))
    slot_p = target - owner_f * capacity + 1.0
    owner_atm = jnp.floor((owner_f + 0.5) * (1.0 / n_land))
    owner_land = owner_f - owner_atm * n_land
    step = owner_land - lnd.astype(F32)
    step = jnp.where(step < 0.0, step + n_land, step)
    turn = owner_atm - atm.astype(F32) - step + (n_land + n_atm)
    turn = turn - jnp.floor((turn + 0.5) * (1.0 / n_atm)) * n_atm
    order = (turn * n_land + step).astype(jnp.int32)
    owner_hot = hot(iota((n, columns), 0) == order)
    owner_bf = owner_hot.astype(BF16)
    block = min(256, columns)
    upper = hot(iota((block, block), 0) <= iota((block, block), 1)).astype(BF16)
    running = jnp.zeros((n, 1), F32)
    ranks = []
    for b in range(columns // block):
        part = slice(b * block, (b + 1) * block)
        seen = dot(owner_bf[:, part], upper)
        ranks.append(jnp.sum(owner_hot[:, part] * (seen + running), axis=0, keepdims=True) - 1.0)
        running = running + seen[:, block - 1 : block]
    rank = jnp.concatenate(ranks, axis=1).astype(jnp.int32)
    place = hot(iota((HALF, columns), 0) == rank)
    high = jnp.floor(slot_p * (1.0 / 64.0))
    low = slot_p - 64.0 * high
    both = jnp.concatenate([(place * high).astype(BF16), (place * low).astype(BF16)], axis=0)
    slot_rows = dot_nt(owner_bf, both)
    tile = tile_ref[...]
    gap = gap_ref[...]
    gap_1 = gap.astype(BF16).astype(F32)
    gap_2 = (gap - gap_1).astype(BF16).astype(F32)
    gap_3 = gap - gap_1 - gap_2
    short = place[:rows]
    tile_of = dot_nt((short * (tile.astype(F32) + 1.0)).astype(BF16), owner_bf)
    gap_of = (
        dot_nt((short * gap_1).astype(BF16), owner_bf)
        + dot_nt((short * gap_2).astype(BF16), owner_bf)
    ) + dot_nt((short * gap_3).astype(BF16), owner_bf)
    return slot_rows, tile_of, gap_of


def net(x_ref, hid, low, act, gains, w_in, w_up, w_down, w_out, width, fill):
    hidden = hid.shape[1]
    parts = [slice(i * width, (i + 1) * width) for i in range(hidden // width)]
    x = x_ref[...]
    total = None
    for c in parts:
        h = dot(x, w_in[:, c])
        hid[:, c] = h
        low[:, c] = (h * gains[0:1, c]).astype(BF16)
        s = jnp.sum(h * h, axis=1, keepdims=True)
        total = s if total is None else total + s
        fill()
    half = lax.rsqrt(total * (1.0 / hidden) + 1e-6) * 0.5
    for c in parts:
        v = dot(low[...], w_up[:, c]) * half
        act[:, c] = (v + v * jnp.tanh(v)).astype(BF16)
        fill()
    total = None
    for c in parts:
        h = hid[:, c] + dot(act[...], w_down[:, c])
        low[:, c] = (h * gains[1:2, c]).astype(BF16)
        s = jnp.sum(h * h, axis=1, keepdims=True)
        total = s if total is None else total + s
        fill()
    scale = lax.rsqrt(total * (1.0 / hidden) + 1e-6)
    return dot(low[...], w_out[...]) * scale


def main_kernel(
    sizes, per_peer, rows, capacity, width,
    tf_hbm, gap_hbm, lapse_hbm, tile_hbm, target_hbm,
    land_hbm, gains_hbm, w_in_hbm, w_up_hbm, w_down_hbm, w_out_hbm,
    fresh_ref, got_slots, flux_ref, hots_ref, counts_ref,
    tf, gap, lapse, tile, target, land, gains, w_in, w_up, w_down, w_out,
    send, slot_rows, tile_of, gap_of, got, slots_s, ahead_state, state, forcing, x, hid, low, act,
    flux, back, load_sem, send_sem, recv_sem, back_send, back_recv, smem_sem,
):
    n_atm, n_land = sizes
    n = n_atm * n_land
    group = n_land
    tiles = tf.shape[0]
    atm = lax.axis_index("atm")
    lnd = lax.axis_index("land")
    block = group * per_peer
    last = n_atm - 1
    message = pl.ds(0, -(-(per_peer + 1) // 2) * 2)

    def atm_ahead(g, p):
        return lax.rem(atm + g + p, n_atm)

    def atm_behind(g, p):
        return lax.rem(atm - g - p + n_atm + n_land + n_atm, n_atm)

    lands_ahead = [lax.rem(lnd + p, n_land) for p in range(n_land)]
    lands_behind = [lax.rem(lnd - p + n_land, n_land) for p in range(n_land)]

    barrier = pltpu.get_barrier_semaphore()

    def greet(g, carry):
        for p in range(group):
            def hello():
                pl.semaphore_signal(
                    barrier, inc=1, device_id=(atm_ahead(g, p), lands_ahead[p]), device_id_type=MESH
                )

            if p == 0:
                pl.when(g > 0)(hello)
            else:
                hello()
        return carry

    loads = [
        pltpu.make_async_copy(src, dst, load_sem.at[i])
        for i, (src, dst) in enumerate(
            [
                (target_hbm, target),
                (tile_hbm, tile),
                (gap_hbm, gap),
                (lapse_hbm, lapse),
                (tf_hbm, tf),
                (land_hbm, land.at[pl.ds(0, capacity)]),
                (gains_hbm, gains),
                (w_in_hbm, w_in),
                (w_up_hbm, w_up),
                (w_down_hbm, w_down),
                (w_out_hbm, w_out),
            ]
        )
    ]
    for load in loads:
        load.start()
    spare = rows - 16
    flux_ref[:, spare:, :] = jnp.zeros((n, 16, LANES), BF16)
    lax.fori_loop(0, n_atm, greet, 0)
    land[pl.ds(capacity, 8), :] = jnp.zeros((8, LANES), F32)
    flux[pl.ds(block, 8), :] = jnp.zeros((8, LANES), F32)
    for load in loads[:5]:
        load.wait()
    slot_rows[...], tile_of[...], gap_of[...] = tables(
        sizes, atm, lnd, per_peer, rows, capacity, gap, tile, target
    )
    lane = iota((rows, tiles), 1).astype(F32) + 1.0
    last_row = hot(iota((rows, LANES), 0) == per_peer)

    def build(g):
        base = g * group
        turn = lax.rem(n - base, n)
        tile_now = pltpu.roll(tile_of[...], turn, axis=1)
        gap_now = pltpu.roll(gap_of[...], turn, axis=1)
        slot_now = slot_rows[pl.ds(pl.multiple_of(base, group), group), :]
        hots = jnp.concatenate(
            [hot(lane == tile_now[:, i : i + 1]).astype(BF16) for i in range(group)], axis=0
        )
        extra = jnp.concatenate(
            [
                gap_now[:, i : i + 1] * lapse[...] + last_row * slot_now[i : i + 1, :]
                for i in range(group)
            ],
            axis=0,
        )
        made = (dot(hots, tf[...]) + extra).astype(BF16)
        spot = pl.ds(base, group)
        hots_ref[spot] = hots.reshape(group, rows, tiles)
        send[spot] = made.reshape(group, rows, LANES)

    def dispatch(g):
        for p in range(group):
            def go():
                pltpu.make_async_remote_copy(
                    src_ref=send.at[g * group + p, message],
                    dst_ref=got.at[g * group + p, message],
                    send_sem=send_sem, recv_sem=recv_sem.at[g],
                    device_id=(atm_ahead(g, p), lands_ahead[p]), device_id_type=MESH,
                ).start()

            if p == 0:
                pl.when(g > 0)(go)
            else:
                go()

    def loop(step):
        def body(g, carry):
            step(g)
            return carry

        lax.fori_loop(0, n_atm, body, 0)

    loop(build)
    got[0] = send[0]
    pl.semaphore_wait(barrier, n - 1)
    loop(dispatch)
    number = jnp.sum(hot(iota((tiles, tile.shape[1]), 0) == tile[...]), axis=1, keepdims=True)
    counts_ref[...] = jnp.broadcast_to(jnp.maximum(number, 1.0), counts_ref.shape)

    def many(ref, start, count, sending, receiving):
        spot = ref.at[pl.ds(start, count), message]
        return pltpu.make_async_remote_copy(
            src_ref=spot, dst_ref=spot, send_sem=sending, recv_sem=receiving,
            device_id=(atm, lands_ahead[1]), device_id_type=MESH,
        )

    def to_smem(g):
        spot = pl.ds(g * group, group)
        return pltpu.make_async_copy(got_slots.at[spot], slots_s.at[spot], smem_sem.at[lax.rem(g, 2)])

    base_row = per_peer // 16 * 16

    def decode(g):
        for p in range(group):
            tail = got[g * group + p, pl.ds(base_row, 16), :].astype(F32)
            row = tail[per_peer - base_row : per_peer - base_row + 1, :]
            slot = row * 64.0 + pltpu.roll(row, HALF, axis=1) - 1.0
            got_slots[g * group + p] = jnp.where(slot < 0.0, float(capacity), slot).astype(jnp.int32)
        to_smem(g).start()

    def fetch(peer, p, k):
        slot = jnp.clip(slots_s[peer, 0, k], 0, capacity)
        ahead_state[pl.ds(p * per_peer + k, 1), :] = land[pl.ds(slot, 1), :]

    def fetch_all(p, carry):
        for k in range(per_peer):
            fetch(p, p, k)
        return carry

    many(got, 1, group - 1, send_sem, recv_sem.at[0]).wait_recv()
    decode(0)
    for load in loads[5:]:
        load.wait()
    to_smem(0).wait()
    lax.fori_loop(0, group, fetch_all, 0)
    if last > 0:
        many(got, group, group, send_sem, recv_sem.at[1]).wait_recv()
        decode(1)

    def chunk(g, carry):
        first = g * group

        @pl.when((g > 0) & (g < last - 1))
        def _():
            many(got, first + 2 * group, group, send_sem, recv_sem.at[g + 2]).wait_recv()
            decode(g + 2)

        @pl.when(g < last)
        def _():
            to_smem(g + 1).wait()

        for p in range(group):
            forcing[pl.ds(p * per_peer, per_peer), :] = got[first + p, :per_peer, :].astype(F32)
        x[:, :LANES] = forcing[...].astype(BF16)
        now = ahead_state[...]
        state[...] = now
        x[:, LANES:] = now.astype(BF16)
        following = jnp.minimum(first + group, n - group)
        todo = [(p, k) for p in range(group) for k in range(per_peer)]
        share = -(-len(todo) // (3 * (hid.shape[1] // width)))

        def fill():
            for p, k in todo[:share]:
                fetch(following + p, p, k)
            del todo[:share]

        result = net(x, hid, low, act, gains, w_in, w_up, w_down, w_out, width, fill)
        tendency = result[:, :LANES].astype(BF16).astype(F32)
        fresh_ref[pl.ds(pl.multiple_of(g * block, 8), block), :] = state[...] + tendency
        flux[pl.ds(0, block), :] = result[:, LANES:]
        for p in range(group):
            back[first + p] = flux[pl.ds(p * per_peer, rows), :].astype(BF16)
        for p in range(group):
            def give():
                a = atm_behind(g, p)
                pltpu.make_async_remote_copy(
                    src_ref=back.at[first + p, message], dst_ref=flux_ref.at[first + p, message],
                    send_sem=back_send, recv_sem=back_recv,
                    device_id=(a, lands_behind[p]), device_id_type=MESH,
                ).start()

            if p == 0:
                pl.when(g > 0)(give)
            else:
                give()

        if last > 1:

            @pl.when(g == 0)
            def _():
                many(got, 2 * group, group, send_sem, recv_sem.at[2]).wait_recv()
                decode(2)

        return carry

    lax.fori_loop(0, n_atm, chunk, 0)
    flux_ref[0] = back[0]
    many(got, 1, n - 1, send_sem, recv_sem.at[0]).wait_send()
    many(back, 1, n - 1, back_send, back_recv).wait_send()
    many(back, 1, n - 1, back_send, back_recv).wait_recv()


def finish_kernel(n, per_peer, capacity, slots_hbm, fresh_ref, flux_ref, hots_ref, counts_ref,
                  state_ref, tile_ref, out, slots_ref, sem, smem_sem):
    parts = 4
    span = n // parts
    unroll = min(8, span)
    copies = [
        pltpu.make_async_copy(
            slots_hbm.at[pl.ds(i * span, span)], slots_ref.at[pl.ds(i * span, span)], smem_sem.at[i]
        )
        for i in range(parts)
    ]
    for copy in copies:
        copy.start()
    total = hots_ref.shape[0]
    step = total // 8
    acc = None
    for i in range(8):
        part = slice(i * step, (i + 1) * step)
        t = dot_tn(hots_ref[part, :], flux_ref[part, :])
        acc = t if acc is None else acc + t
    tile_ref[...] = acc / counts_ref[...]

    def clear(i, carry):
        out[pl.ds(i * 64, 64), :] = jnp.zeros((64, LANES), F32)
        return carry

    lax.fori_loop(0, capacity // 64, clear, 0)
    if capacity % 64:
        out[pl.ds(capacity // 64 * 64, capacity % 64), :] = jnp.zeros((capacity % 64, LANES), F32)

    def place(i, carry):
        for u in range(unroll):
            d = i * unroll + u
            for k in range(per_peer):
                slot = slots_ref[d, 0, k]
                out[pl.ds(slot, 1), :] = fresh_ref[pl.ds(d * per_peer + k, 1), :]
        return carry

    for i in range(parts):
        copies[i].wait()
        lax.fori_loop(i * span // unroll, (i + 1) * span // unroll, place, 0)
    copy = pltpu.make_async_copy(out.at[pl.ds(0, capacity)], state_ref, sem)
    copy.start()
    copy.wait()


def limit(mib):
    return pltpu.CompilerParams(vmem_limit_bytes=mib * 1024 * 1024)


def local(
    sizes, tile_forcing, elevation_gap, lapse_rate, column_tile, column_target, owner_counts,
    land_state, w_in, norm_gains, w_up, w_down, w_out,
):
    n = sizes[0] * sizes[1]
    capacity = land_state.shape[0]
    per_peer = capacity // n + 1
    rows = -(-per_peer // 16) * 16
    columns = elevation_gap.shape[0]
    tiles, features = tile_forcing.shape
    hidden = w_in.shape[1]
    group = sizes[1]
    block = group * per_peer
    S = jax.ShapeDtypeStruct
    dma = pltpu.SemaphoreType.DMA
    fresh, got_slots, flux, hots, counts = pl.pallas_call(
        functools.partial(main_kernel, sizes, per_peer, rows, capacity, min(hidden, 1024)),
        out_shape=[
            S((n * per_peer, features), F32), S((n, 1, LANES), jnp.int32), S((n, rows, features), BF16),
            S((n, rows, tiles), BF16), S((tiles, features), F32),
        ],
        in_specs=[HBM] * 11,
        out_specs=[VMEM] * 5,
        scratch_shapes=[
            pltpu.VMEM((tiles, features), BF16),
            pltpu.VMEM((1, columns), F32),
            pltpu.VMEM((1, features), F32),
            pltpu.VMEM((1, columns), jnp.int32),
            pltpu.VMEM((1, columns), jnp.int32),
            pltpu.VMEM((capacity + 8, features), F32),
            pltpu.VMEM(norm_gains.shape, F32),
            pltpu.VMEM(w_in.shape, BF16),
            pltpu.VMEM(w_up.shape[1:], BF16),
            pltpu.VMEM(w_down.shape[1:], BF16),
            pltpu.VMEM(w_out.shape, BF16),
            pltpu.VMEM((n, rows, features), BF16),
            pltpu.VMEM((n, LANES), F32),
            pltpu.VMEM((rows, n), F32),
            pltpu.VMEM((rows, n), F32),
            pltpu.VMEM((n, rows, features), BF16),
            pltpu.SMEM((n, 1, LANES), jnp.int32),
            pltpu.VMEM((block, features), F32),
            pltpu.VMEM((block, features), F32),
            pltpu.VMEM((block, features), F32),
            pltpu.VMEM((block, 2 * features), BF16),
            pltpu.VMEM((block, hidden), F32),
            pltpu.VMEM((block, hidden), BF16),
            pltpu.VMEM((block, hidden), BF16),
            pltpu.VMEM((block + 8, features), F32),
            pltpu.VMEM((n, rows, features), BF16),
            dma((11,)), dma(()), dma((n // group,)), dma(()), dma(()), dma((2,)),
        ],
        compiler_params=pltpu.CompilerParams(
            collective_id=0, has_side_effects=True, vmem_limit_bytes=40 * 1024 * 1024
        ),
        name="exchange",
    )(
        *[
            pltpu.with_memory_space_constraint(v, pltpu.HBM)
            for v in (
                tile_forcing, elevation_gap.reshape(1, columns), lapse_rate.reshape(1, features),
                column_tile.reshape(1, columns), column_target.reshape(1, columns),
                land_state, norm_gains, w_in, w_up[0], w_down[0], w_out,
            )
        ]
    )
    return pl.pallas_call(
        functools.partial(finish_kernel, n, per_peer, capacity),
        out_shape=[S((capacity, features), F32), S((tiles, features), F32)],
        in_specs=[VMEM] * 5,
        out_specs=[ANY, VMEM],
        scratch_shapes=[
            pltpu.VMEM((capacity + 8, features), F32), pltpu.SMEM((n, 1, LANES), jnp.int32),
            dma(()), dma((4,)),
        ],
        compiler_params=limit(24),
        name="finish",
    )(
        got_slots, fresh, flux.reshape(n * rows, features), hots.reshape(n * rows, tiles), counts
    )


def solution(mesh):
    both = P(("atm", "land"))
    wide = P(("atm", "land"), None)
    sizes = (mesh.shape["atm"], mesh.shape["land"])
    return jax.shard_map(
        functools.partial(local, sizes),
        mesh=mesh,
        in_specs=(wide, both, P(), both, both, both, wide, P(), P(), P(), P(), P()),
        out_specs=(wide, wide),
        check_vma=False,
    )
```

```python
import functools

import jax
import jax.numpy as jnp
from jax import lax
from jax.experimental import pallas as pl
from jax.experimental.pallas import tpu as pltpu
from jax.sharding import PartitionSpec as P

F32 = jnp.float32
BF16 = jnp.bfloat16
LANES = 128
HALF = 64
VMEM = pl.BlockSpec(memory_space=pltpu.VMEM)
HBM = pl.BlockSpec(memory_space=pltpu.HBM)
ANY = pl.BlockSpec(memory_space=pl.ANY)
MESH = pl.DeviceIdType.MESH


def dot(a, b):
    return jnp.dot(a, b, preferred_element_type=F32)


def dot_nt(a, b):
    return lax.dot_general(a, b, (((1,), (1,)), ((), ())), preferred_element_type=F32)


def dot_tn(a, b):
    return lax.dot_general(a, b, (((0,), (0,)), ((), ())), preferred_element_type=F32)


def iota(shape, dim):
    return lax.broadcasted_iota(jnp.int32, shape, dim)


def hot(mask):
    return jnp.where(mask, 1.0, 0.0)


def tables(sizes, atm, lnd, per_peer, rows, capacity, gap_ref, tile_ref, target_ref):
    n_atm, n_land = sizes
    n = n_atm * n_land
    columns = target_ref.shape[1]
    target = target_ref[...].astype(F32)
    owner_f = jnp.floor((target + 0.5) * (1.0 / capacity))
    slot_p = target - owner_f * capacity + 1.0
    owner_atm = jnp.floor((owner_f + 0.5) * (1.0 / n_land))
    owner_land = owner_f - owner_atm * n_land
    step = owner_land - lnd.astype(F32)
    step = jnp.where(step < 0.0, step + n_land, step)
    turn = owner_atm - atm.astype(F32) - 3.0 * step + (3 * n_land + n_atm)
    turn = turn - jnp.floor((turn + 0.5) * (1.0 / n_atm)) * n_atm
    order = (turn * n_land + step).astype(jnp.int32)
    owner_hot = hot(iota((n, columns), 0) == order)
    owner_bf = owner_hot.astype(BF16)
    block = min(256, columns)
    upper = hot(iota((block, block), 0) <= iota((block, block), 1)).astype(BF16)
    running = jnp.zeros((n, 1), F32)
    ranks = []
    for b in range(columns // block):
        part = slice(b * block, (b + 1) * block)
        seen = dot(owner_bf[:, part], upper)
        ranks.append(jnp.sum(owner_hot[:, part] * (seen + running), axis=0, keepdims=True) - 1.0)
        running = running + seen[:, block - 1 : block]
    rank = jnp.concatenate(ranks, axis=1).astype(jnp.int32)
    place = hot(iota((HALF, columns), 0) == rank)
    high = jnp.floor(slot_p * (1.0 / 64.0))
    low = slot_p - 64.0 * high
    both = jnp.concatenate([(place * high).astype(BF16), (place * low).astype(BF16)], axis=0)
    slot_rows = dot_nt(owner_bf, both)
    tile = tile_ref[...]
    gap = gap_ref[...]
    gap_1 = gap.astype(BF16).astype(F32)
    gap_2 = (gap - gap_1).astype(BF16).astype(F32)
    gap_3 = gap - gap_1 - gap_2
    short = place[:rows]
    tile_of = dot_nt((short * (tile.astype(F32) + 1.0)).astype(BF16), owner_bf)
    gap_of = (
        dot_nt((short * gap_1).astype(BF16), owner_bf)
        + dot_nt((short * gap_2).astype(BF16), owner_bf)
    ) + dot_nt((short * gap_3).astype(BF16), owner_bf)
    return slot_rows, tile_of, gap_of


def net(x_ref, hid, low, act, gains, w_in, w_up, w_down, w_out, width, fill):
    hidden = hid.shape[1]
    parts = [slice(i * width, (i + 1) * width) for i in range(hidden // width)]
    x = x_ref[...]
    total = None
    for c in parts:
        h = dot(x, w_in[:, c])
        hid[:, c] = h
        low[:, c] = (h * gains[0:1, c]).astype(BF16)
        s = jnp.sum(h * h, axis=1, keepdims=True)
        total = s if total is None else total + s
        fill()
    half = lax.rsqrt(total * (1.0 / hidden) + 1e-6) * 0.5
    for c in parts:
        v = dot(low[...], w_up[:, c]) * half
        act[:, c] = (v + v * jnp.tanh(v)).astype(BF16)
        fill()
    total = None
    for c in parts:
        h = hid[:, c] + dot(act[...], w_down[:, c])
        low[:, c] = (h * gains[1:2, c]).astype(BF16)
        s = jnp.sum(h * h, axis=1, keepdims=True)
        total = s if total is None else total + s
        fill()
    scale = lax.rsqrt(total * (1.0 / hidden) + 1e-6)
    return dot(low[...], w_out[...]) * scale


def main_kernel(
    sizes, per_peer, rows, capacity, width,
    tf_hbm, gap_hbm, lapse_hbm, tile_hbm, target_hbm,
    land_hbm, gains_hbm, w_in_hbm, w_up_hbm, w_down_hbm, w_out_hbm,
    fresh_ref, got_slots, flux_ref, hots_ref, counts_ref,
    tf, gap, lapse, tile, target, land, gains, w_in, w_up, w_down, w_out,
    send, slot_rows, tile_of, gap_of, got, slots_s, ahead_state, state, forcing, x, hid, low, act,
    flux, back, load_sem, send_sem, recv_sem, back_send, back_recv, smem_sem,
):
    n_atm, n_land = sizes
    n = n_atm * n_land
    group = n_land
    tiles = tf.shape[0]
    atm = lax.axis_index("atm")
    lnd = lax.axis_index("land")
    block = group * per_peer
    last = n_atm - 1
    message = pl.ds(0, -(-(per_peer + 1) // 2) * 2)

    def atm_ahead(g, p):
        return lax.rem(atm + g + 3 * p, n_atm)

    def atm_behind(g, p):
        return lax.rem(atm - g - 3 * p + n_atm + 3 * n_land + n_atm, n_atm)

    lands_ahead = [lax.rem(lnd + p, n_land) for p in range(n_land)]
    lands_behind = [lax.rem(lnd - p + n_land, n_land) for p in range(n_land)]

    barrier = pltpu.get_barrier_semaphore()

    def greet(g, carry):
        for p in range(group):
            def hello():
                pl.semaphore_signal(
                    barrier, inc=1, device_id=(atm_ahead(g, p), lands_ahead[p]), device_id_type=MESH
                )

            if p == 0:
                pl.when(g > 0)(hello)
            else:
                hello()
        return carry

    loads = [
        pltpu.make_async_copy(src, dst, load_sem.at[i])
        for i, (src, dst) in enumerate(
            [
                (target_hbm, target),
                (tile_hbm, tile),
                (gap_hbm, gap),
                (lapse_hbm, lapse),
                (tf_hbm, tf),
                (land_hbm, land.at[pl.ds(0, capacity)]),
                (gains_hbm, gains),
                (w_in_hbm, w_in),
                (w_up_hbm, w_up),
                (w_down_hbm, w_down),
                (w_out_hbm, w_out),
            ]
        )
    ]
    for load in loads:
        load.start()
    spare = rows - 16
    flux_ref[:, spare:, :] = jnp.zeros((n, 16, LANES), BF16)
    lax.fori_loop(0, n_atm, greet, 0)
    land[pl.ds(capacity, 8), :] = jnp.zeros((8, LANES), F32)
    flux[pl.ds(block, 8), :] = jnp.zeros((8, LANES), F32)
    for load in loads[:5]:
        load.wait()
    slot_rows[...], tile_of[...], gap_of[...] = tables(
        sizes, atm, lnd, per_peer, rows, capacity, gap, tile, target
    )
    lane = iota((rows, tiles), 1).astype(F32) + 1.0
    last_row = hot(iota((rows, LANES), 0) == per_peer)

    def build(g):
        base = g * group
        turn = lax.rem(n - base, n)
        tile_now = pltpu.roll(tile_of[...], turn, axis=1)
        gap_now = pltpu.roll(gap_of[...], turn, axis=1)
        slot_now = slot_rows[pl.ds(pl.multiple_of(base, group), group), :]
        hots = jnp.concatenate(
            [hot(lane == tile_now[:, i : i + 1]).astype(BF16) for i in range(group)], axis=0
        )
        extra = jnp.concatenate(
            [
                gap_now[:, i : i + 1] * lapse[...] + last_row * slot_now[i : i + 1, :]
                for i in range(group)
            ],
            axis=0,
        )
        made = (dot(hots, tf[...]) + extra).astype(BF16)
        spot = pl.ds(base, group)
        hots_ref[spot] = hots.reshape(group, rows, tiles)
        send[spot] = made.reshape(group, rows, LANES)

    def dispatch(g):
        for p in range(group):
            def go():
                pltpu.make_async_remote_copy(
                    src_ref=send.at[g * group + p, message],
                    dst_ref=got.at[g * group + p, message],
                    send_sem=send_sem, recv_sem=recv_sem.at[g],
                    device_id=(atm_ahead(g, p), lands_ahead[p]), device_id_type=MESH,
                ).start()

            if p == 0:
                pl.when(g > 0)(go)
            else:
                go()

    def loop(step):
        def body(g, carry):
            step(g)
            return carry

        lax.fori_loop(0, n_atm, body, 0)

    loop(build)
    got[0] = send[0]
    pl.semaphore_wait(barrier, n - 1)
    loop(dispatch)
    number = jnp.sum(hot(iota((tiles, tile.shape[1]), 0) == tile[...]), axis=1, keepdims=True)
    counts_ref[...] = jnp.broadcast_to(jnp.maximum(number, 1.0), counts_ref.shape)

    def many(ref, start, count, sending, receiving):
        spot = ref.at[pl.ds(start, count), message]
        return pltpu.make_async_remote_copy(
            src_ref=spot, dst_ref=spot, send_sem=sending, recv_sem=receiving,
            device_id=(atm, lands_ahead[1]), device_id_type=MESH,
        )

    def to_smem(g):
        spot = pl.ds(g * group, group)
        return pltpu.make_async_copy(got_slots.at[spot], slots_s.at[spot], smem_sem.at[lax.rem(g, 2)])

    base_row = per_peer // 16 * 16

    def decode(g):
        for p in range(group):
            tail = got[g * group + p, pl.ds(base_row, 16), :].astype(F32)
            row = tail[per_peer - base_row : per_peer - base_row + 1, :]
            slot = row * 64.0 + pltpu.roll(row, HALF, axis=1) - 1.0
            got_slots[g * group + p] = jnp.where(slot < 0.0, float(capacity), slot).astype(jnp.int32)
        to_smem(g).start()

    def fetch(peer, p, k):
        slot = jnp.clip(slots_s[peer, 0, k], 0, capacity)
        ahead_state[pl.ds(p * per_peer + k, 1), :] = land[pl.ds(slot, 1), :]

    def fetch_all(p, carry):
        for k in range(per_peer):
            fetch(p, p, k)
        return carry

    many(got, 1, group - 1, send_sem, recv_sem.at[0]).wait_recv()
    decode(0)
    for load in loads[5:]:
        load.wait()
    to_smem(0).wait()
    lax.fori_loop(0, group, fetch_all, 0)
    if last > 0:
        many(got, group, group, send_sem, recv_sem.at[1]).wait_recv()
        decode(1)

    def chunk(g, carry):
        first = g * group

        @pl.when((g > 0) & (g < last - 1))
        def _():
            many(got, first + 2 * group, group, send_sem, recv_sem.at[g + 2]).wait_recv()
            decode(g + 2)

        @pl.when(g < last)
        def _():
            to_smem(g + 1).wait()

        for p in range(group):
            forcing[pl.ds(p * per_peer, per_peer), :] = got[first + p, :per_peer, :].astype(F32)
        x[:, :LANES] = forcing[...].astype(BF16)
        now = ahead_state[...]
        state[...] = now
        x[:, LANES:] = now.astype(BF16)
        following = jnp.minimum(first + group, n - group)
        todo = [(p, k) for p in range(group) for k in range(per_peer)]
        share = -(-len(todo) // (3 * (hid.shape[1] // width)))

        def fill():
            for p, k in todo[:share]:
                fetch(following + p, p, k)
            del todo[:share]

        result = net(x, hid, low, act, gains, w_in, w_up, w_down, w_out, width, fill)
        tendency = result[:, :LANES].astype(BF16).astype(F32)
        fresh_ref[pl.ds(pl.multiple_of(g * block, 8), block), :] = state[...] + tendency
        flux[pl.ds(0, block), :] = result[:, LANES:]
        for p in range(group):
            back[first + p] = flux[pl.ds(p * per_peer, rows), :].astype(BF16)
        for p in range(group):
            def give():
                a = atm_behind(g, p)
                pltpu.make_async_remote_copy(
                    src_ref=back.at[first + p, message], dst_ref=flux_ref.at[first + p, message],
                    send_sem=back_send, recv_sem=back_recv,
                    device_id=(a, lands_behind[p]), device_id_type=MESH,
                ).start()

            if p == 0:
                pl.when(g > 0)(give)
            else:
                give()

        if last > 1:

            @pl.when(g == 0)
            def _():
                many(got, 2 * group, group, send_sem, recv_sem.at[2]).wait_recv()
                decode(2)

        return carry

    lax.fori_loop(0, n_atm, chunk, 0)
    flux_ref[0] = back[0]
    many(got, 1, n - 1, send_sem, recv_sem.at[0]).wait_send()
    many(back, 1, n - 1, back_send, back_recv).wait_send()
    many(back, 1, n - 1, back_send, back_recv).wait_recv()


def finish_kernel(n, per_peer, capacity, slots_hbm, fresh_ref, flux_ref, hots_ref, counts_ref,
                  state_ref, tile_ref, out, slots_ref, sem, smem_sem):
    parts = 4
    span = n // parts
    unroll = min(8, span)
    copies = [
        pltpu.make_async_copy(
            slots_hbm.at[pl.ds(i * span, span)], slots_ref.at[pl.ds(i * span, span)], smem_sem.at[i]
        )
        for i in range(parts)
    ]
    for copy in copies:
        copy.start()
    total = hots_ref.shape[0]
    step = total // 8
    acc = None
    for i in range(8):
        part = slice(i * step, (i + 1) * step)
        t = dot_tn(hots_ref[part, :], flux_ref[part, :])
        acc = t if acc is None else acc + t
    tile_ref[...] = acc / counts_ref[...]

    def clear(i, carry):
        out[pl.ds(i * 64, 64), :] = jnp.zeros((64, LANES), F32)
        return carry

    lax.fori_loop(0, capacity // 64, clear, 0)
    if capacity % 64:
        out[pl.ds(capacity // 64 * 64, capacity % 64), :] = jnp.zeros((capacity % 64, LANES), F32)

    def place(i, carry):
        for u in range(unroll):
            d = i * unroll + u
            for k in range(per_peer):
                slot = slots_ref[d, 0, k]
                out[pl.ds(slot, 1), :] = fresh_ref[pl.ds(d * per_peer + k, 1), :]
        return carry

    for i in range(parts):
        copies[i].wait()
        lax.fori_loop(i * span // unroll, (i + 1) * span // unroll, place, 0)
    copy = pltpu.make_async_copy(out.at[pl.ds(0, capacity)], state_ref, sem)
    copy.start()
    copy.wait()


def limit(mib):
    return pltpu.CompilerParams(vmem_limit_bytes=mib * 1024 * 1024)


def local(
    sizes, tile_forcing, elevation_gap, lapse_rate, column_tile, column_target, owner_counts,
    land_state, w_in, norm_gains, w_up, w_down, w_out,
):
    n = sizes[0] * sizes[1]
    capacity = land_state.shape[0]
    per_peer = capacity // n + 1
    rows = -(-per_peer // 16) * 16
    columns = elevation_gap.shape[0]
    tiles, features = tile_forcing.shape
    hidden = w_in.shape[1]
    group = sizes[1]
    block = group * per_peer
    S = jax.ShapeDtypeStruct
    dma = pltpu.SemaphoreType.DMA
    fresh, got_slots, flux, hots, counts = pl.pallas_call(
        functools.partial(main_kernel, sizes, per_peer, rows, capacity, min(hidden, 1024)),
        out_shape=[
            S((n * per_peer, features), F32), S((n, 1, LANES), jnp.int32), S((n, rows, features), BF16),
            S((n, rows, tiles), BF16), S((tiles, features), F32),
        ],
        in_specs=[HBM] * 11,
        out_specs=[VMEM] * 5,
        scratch_shapes=[
            pltpu.VMEM((tiles, features), BF16),
            pltpu.VMEM((1, columns), F32),
            pltpu.VMEM((1, features), F32),
            pltpu.VMEM((1, columns), jnp.int32),
            pltpu.VMEM((1, columns), jnp.int32),
            pltpu.VMEM((capacity + 8, features), F32),
            pltpu.VMEM(norm_gains.shape, F32),
            pltpu.VMEM(w_in.shape, BF16),
            pltpu.VMEM(w_up.shape[1:], BF16),
            pltpu.VMEM(w_down.shape[1:], BF16),
            pltpu.VMEM(w_out.shape, BF16),
            pltpu.VMEM((n, rows, features), BF16),
            pltpu.VMEM((n, LANES), F32),
            pltpu.VMEM((rows, n), F32),
            pltpu.VMEM((rows, n), F32),
            pltpu.VMEM((n, rows, features), BF16),
            pltpu.SMEM((n, 1, LANES), jnp.int32),
            pltpu.VMEM((block, features), F32),
            pltpu.VMEM((block, features), F32),
            pltpu.VMEM((block, features), F32),
            pltpu.VMEM((block, 2 * features), BF16),
            pltpu.VMEM((block, hidden), F32),
            pltpu.VMEM((block, hidden), BF16),
            pltpu.VMEM((block, hidden), BF16),
            pltpu.VMEM((block + 8, features), F32),
            pltpu.VMEM((n, rows, features), BF16),
            dma((11,)), dma(()), dma((n // group,)), dma(()), dma(()), dma((2,)),
        ],
        compiler_params=pltpu.CompilerParams(
            collective_id=0, has_side_effects=True, vmem_limit_bytes=40 * 1024 * 1024
        ),
        name="exchange",
    )(
        *[
            pltpu.with_memory_space_constraint(v, pltpu.HBM)
            for v in (
                tile_forcing, elevation_gap.reshape(1, columns), lapse_rate.reshape(1, features),
                column_tile.reshape(1, columns), column_target.reshape(1, columns),
                land_state, norm_gains, w_in, w_up[0], w_down[0], w_out,
            )
        ]
    )
    return pl.pallas_call(
        functools.partial(finish_kernel, n, per_peer, capacity),
        out_shape=[S((capacity, features), F32), S((tiles, features), F32)],
        in_specs=[VMEM] * 5,
        out_specs=[ANY, VMEM],
        scratch_shapes=[
            pltpu.VMEM((capacity + 8, features), F32), pltpu.SMEM((n, 1, LANES), jnp.int32),
            dma(()), dma((4,)),
        ],
        compiler_params=limit(24),
        name="finish",
    )(
        got_slots, fresh, flux.reshape(n * rows, features), hots.reshape(n * rows, tiles), counts
    )


def solution(mesh):
    both = P(("atm", "land"))
    wide = P(("atm", "land"), None)
    sizes = (mesh.shape["atm"], mesh.shape["land"])
    return jax.shard_map(
        functools.partial(local, sizes),
        mesh=mesh,
        in_specs=(wide, both, P(), both, both, both, wide, P(), P(), P(), P(), P()),
        out_specs=(wide, wide),
        check_vma=False,
    )
```
